32 devices in a mesh: rhs: 1 (over z), mode1: 4 (over y), mode2: 4 (over x), mode3: 2 (over core).
Axes of the slice: x: 4, y: 4, z: 1, core: 2. Of those that a mesh axis runs over, the one named last changes fastest.
The devices are a block of a 4x4x8 slice.
Arguments:
- x_vol: bfloat16 [2, 512, 256, 512], P('rhs', 'mode1', 'mode2', 'mode3')
- diag_vals: float32 [512, 256, 512], P('mode1', 'mode2', 'mode3')
- a_mode1: bfloat16 [512, 512], replicated
- a_mode2: bfloat16 [256, 256], replicated
- a_mode3: bfloat16 [512, 512], replicated
- b_mode1: bfloat16 [512, 512], replicated
- b_mode2: bfloat16 [256, 256], replicated
- b_mode3: bfloat16 [512, 512], replicated
Outputs:
- output: float32 [2, 512, 256, 512], P('rhs', 'mode1', 'mode2', 'mode3')
All inputs are finite; a program needn't handle non-finite values.
Results may differ from the reference program's by a relative error of at most 0.0109024.
Values are sent between devices in bfloat16 or wider.
A program may use at most 768 MiB of HBM per device.

```python
import jax
import jax.numpy as jnp
from jax import lax

RHS_COUNT = 2
MODE1_LEN = 512
MODE2_LEN = 256
MODE3_LEN = 512


def factor(sub_key, size):
    return (jax.random.normal(sub_key, (size, size), jnp.float32) * (3.0 * size) ** -0.5).astype(jnp.bfloat16)


def setup_inputs(seed: int = 0, part: int = 0) -> dict:
    base_key = jax.random.key(seed)
    key_list = jax.random.split(base_key, 8)
    own_key = jax.random.fold_in(key_list[0], part)
    x_vol = jax.random.normal(own_key, (RHS_COUNT, MODE1_LEN, MODE2_LEN, MODE3_LEN), jnp.float32).astype(jnp.bfloat16)
    diag_vals = 10.0 ** jax.random.uniform(key_list[1], (MODE1_LEN, MODE2_LEN, MODE3_LEN), jnp.float32, -0.5, 0.5)
    return {
        'x_vol': x_vol,
        'diag_vals': diag_vals,
        'a_mode1': factor(key_list[2], MODE1_LEN),
        'a_mode2': factor(key_list[3], MODE2_LEN),
        'a_mode3': factor(key_list[4], MODE3_LEN),
        'b_mode1': factor(key_list[5], MODE1_LEN),
        'b_mode2': factor(key_list[6], MODE2_LEN),
        'b_mode3': factor(key_list[7], MODE3_LEN),
    }


def mode_sum(volume, mat_one, mat_two, mat_three):
    volume_f = volume.astype(jnp.float32)
    term_one = jnp.einsum('ia,ajk->ijk', mat_one.astype(jnp.float32), volume_f).astype(jnp.bfloat16)
    term_two = jnp.einsum('jb,ibk->ijk', mat_two.astype(jnp.float32), volume_f).astype(jnp.bfloat16)
    term_three = jnp.einsum('ijc,kc->ijk', volume_f, mat_three.astype(jnp.float32)).astype(jnp.bfloat16)
    return term_one.astype(jnp.float32) + term_two.astype(jnp.float32) + term_three.astype(jnp.float32)


def reference(x_vol, diag_vals, a_mode1, a_mode2, a_mode3, b_mode1, b_mode2, b_mode3):
    def apply_one(volume):
        u_vol = mode_sum(volume, a_mode1, a_mode2, a_mode3).astype(jnp.bfloat16)
        w_vol = (diag_vals * u_vol.astype(jnp.float32)).astype(jnp.bfloat16)
        return mode_sum(w_vol, b_mode1, b_mode2, b_mode3)
    return lax.map(apply_one, x_vol)
```

```python
import functools

import jax
import jax.numpy as jnp
from jax import lax
from jax.experimental import pallas as pl
from jax.experimental.pallas import tpu as pltpu
from jax.sharding import PartitionSpec as P

MESH = pl.DeviceIdType.MESH
F32, BF16 = jnp.float32, jnp.bfloat16
LANES = 128


def aligned(index, size):
    return pl.ds(pl.multiple_of(index * size, size), size)


def kernel(dims, x_ref, d_ref, a1_ref, a2_ref, a3_ref, b1_ref, b2_ref, b3_ref,
           z_ref, lin1, lin2, lin3, out1, out2, t1, t2, w,
           vin1, vscr, vout1, vin2, vout2, v1, v2, vown, vpar, vd, vw, vz,
           y_send, y_recv, x_send, x_recv, c_send, c_recv,
           y_send2, y_recv2, x_send2, x_recv2, load_sem, store_sem):
    n1, n2, n3, rhs, ni, nj, nk = dims
    halves = nk // LANES
    chunks = rhs * halves
    jc, ic = nj // n1, ni // n2
    me1, me2, me3 = lax.axis_index('mode1'), lax.axis_index('mode2'), lax.axis_index('mode3')
    peer1 = [lax.rem(me1 + s, n1) for s in range(1, n1)]
    peer2 = [lax.rem(me2 + s, n2) for s in range(1, n2)]
    peer3 = lax.rem(me3 + 1, n3)

    barrier = pltpu.get_barrier_semaphore()
    for axis, peers in (('mode1', peer1), ('mode2', peer2), ('mode3', [peer3])):
        for peer in peers:
            pl.semaphore_signal(barrier, inc=1, device_id={axis: peer}, device_id_type=MESH)
    pl.semaphore_wait(barrier, n1 + n2 + n3 - 3)

    def remote(src, dst, send, recv, axis, peer):
        return pltpu.make_async_remote_copy(src_ref=src, dst_ref=dst, send_sem=send, recv_sem=recv,
                                            device_id={axis: peer}, device_id_type=MESH)

    def field(stage, c):
        if stage == 0:
            return x_ref.at[c // halves, :, :, aligned(lax.rem(c, halves), LANES)]
        return w.at[c]

    def out_y(stage, c, n):
        g = stage * chunks + c
        return remote(field(stage, c).at[:, aligned(peer1[n], jc), :], lin1.at[g, aligned(me1, ni)],
                      y_send.at[g, n], y_recv.at[g, n], 'mode1', peer1[n])

    def out_x(stage, c, n):
        g = stage * chunks + c
        return remote(field(stage, c).at[aligned(peer2[n], ic)], lin2.at[g, :, aligned(me2, nj), :],
                      x_send.at[g, n], x_recv.at[g, n], 'mode2', peer2[n])

    def out_c(stage, c):
        g = stage * chunks + c
        return remote(field(stage, c), lin3.at[g], c_send.at[g], c_recv.at[g], 'mode3', peer3)

    def back_y(stage, c, n):
        g = stage * chunks + c
        return remote(out1.at[g, aligned(peer1[n], ni)], t1.at[g, :, aligned(me1, jc), :],
                      y_send2.at[g, n], y_recv2.at[g, n], 'mode1', peer1[n])

    def back_x(stage, c, n):
        g = stage * chunks + c
        return remote(out2.at[g, :, aligned(peer2[n], nj), :], t2.at[g, aligned(me2, ic)],
                      x_send2.at[g, n], x_recv2.at[g, n], 'mode2', peer2[n])

    order1 = sorted(range(n1 - 1), key=lambda n: min(n + 1, n1 - n - 1))
    order2 = sorted(range(n2 - 1), key=lambda n: min(n + 1, n2 - n - 1))

    def start_out(stage, c):
        for n in order1:
            out_y(stage, c, n).start()
        for n in order2:
            out_x(stage, c, n).start()
        out_c(stage, c).start()

    def product_one(stage, c):
        g = stage * chunks + c
        mat = (a1_ref, b1_ref)[stage]
        for n in range(n1 - 1):
            out_y(stage, c, n).wait_recv()
        loads = [pltpu.make_async_copy(field(stage, c).at[:, aligned(me1, jc), :], vin1.at[aligned(me1, ni)], load_sem.at[0])]
        loads += [pltpu.make_async_copy(lin1.at[g, aligned(peer1[n], ni)], vin1.at[aligned(peer1[n], ni)], load_sem.at[n + 1])
                  for n in range(n1 - 1)]
        for copy in loads:
            copy.start()
        for copy in loads:
            copy.wait()
        full = n1 * ni
        part = 32

        @pl.loop(0, full // part)
        def _(b):
            vscr[pl.ds(pl.multiple_of(b * part * jc, part * jc), part * jc), :] = (
                vin1[pl.ds(b * part, part)].astype(F32).reshape(part * jc, LANES))

        @pl.loop(0, jc // 2)
        def _(b):
            rows = [pl.ds(2 * b + h, full, stride=jc) for h in range(2)]
            rhs_mat = jnp.concatenate([vscr[row, :].astype(BF16) for row in rows], axis=1)
            res = jnp.dot(mat[...], rhs_mat, preferred_element_type=F32)
            for h in range(2):
                vscr[rows[h], :] = res[:, h * LANES:(h + 1) * LANES]

        @pl.loop(0, full // part)
        def _(b):
            vout1[pl.ds(b * part, part)] = (
                vscr[pl.ds(pl.multiple_of(b * part * jc, part * jc), part * jc), :].reshape(part, jc, LANES).astype(BF16))

        stores = [pltpu.make_async_copy(vout1.at[aligned(peer1[n], ni)], out1.at[g, aligned(peer1[n], ni)], store_sem.at[n + 1])
                  for n in range(n1 - 1)]
        stores += [pltpu.make_async_copy(vout1.at[aligned(me1, ni)], t1.at[g, :, aligned(me1, jc), :], store_sem.at[0])]
        for copy in stores:
            copy.start()
        for copy in stores:
            copy.wait()
        for n in order1:
            back_y(stage, c, n).start()

    def product_two(stage, c):
        g = stage * chunks + c
        mat = (a2_ref, b2_ref)[stage]
        for n in range(n2 - 1):
            out_x(stage, c, n).wait_recv()
        loads = [pltpu.make_async_copy(field(stage, c).at[aligned(me2, ic)], vin2.at[:, aligned(me2, nj), :], load_sem.at[0])]
        loads += [pltpu.make_async_copy(lin2.at[g, :, aligned(peer2[n], nj), :], vin2.at[:, aligned(peer2[n], nj), :], load_sem.at[n + 1])
                  for n in range(n2 - 1)]
        for copy in loads:
            copy.start()
        for copy in loads:
            copy.wait()

        @pl.loop(0, ic // 2)
        def _(b):
            rhs_mat = jnp.concatenate([vin2[2 * b], vin2[2 * b + 1]], axis=1)
            res = jnp.dot(mat[...], rhs_mat, preferred_element_type=F32).astype(BF16)
            vout2[2 * b] = res[:, :LANES]
            vout2[2 * b + 1] = res[:, LANES:]

        stores = [pltpu.make_async_copy(vout2.at[:, aligned(peer2[n], nj), :], out2.at[g, :, aligned(peer2[n], nj), :], store_sem.at[n + 1])
                  for n in range(n2 - 1)]
        stores += [pltpu.make_async_copy(vout2.at[:, aligned(me2, nj), :], t2.at[g, aligned(me2, ic)], store_sem.at[0])]
        for copy in stores:
            copy.start()
        for copy in stores:
            copy.wait()
        for n in order2:
            back_x(stage, c, n).start()

    def total(stage, c):
        g = stage * chunks + c
        r, half = c // halves, lax.rem(c, halves)
        mat = (a3_ref, b3_ref)[stage]
        for n in range(n1 - 1):
            back_y(stage, c, n).wait_recv()
        for n in range(n2 - 1):
            back_x(stage, c, n).wait_recv()
        loads = [pltpu.make_async_copy(t1.at[g], v1, load_sem.at[0]),
                 pltpu.make_async_copy(t2.at[g], v2, load_sem.at[1])]
        for h in range(halves):
            lanes = pl.ds(h * LANES, LANES)
            loads += [pltpu.make_async_copy(field(stage, r * halves + h), vown.at[:, :, lanes], load_sem.at[2 + h]),
                      pltpu.make_async_copy(lin3.at[stage * chunks + r * halves + h], vpar.at[:, :, lanes], load_sem.at[2 + halves + h])]
        if stage == 0:
            loads += [pltpu.make_async_copy(d_ref.at[:, :, aligned(half, LANES)], vd, load_sem.at[2 + 2 * halves])]
        for copy in loads:
            copy.start()
        for copy in loads:
            copy.wait()
        rows = pl.ds(pl.multiple_of(me3 * nk + half * LANES, LANES), LANES)
        mat_own = mat[rows, aligned(me3, nk)]
        mat_par = mat[rows, aligned(peer3, nk)]
        contract = (((1,), (1,)), ((), ()))
        part = 8

        @pl.loop(0, ni // part)
        def _(b):
            sel = pl.ds(b * part, part)
            term = lax.dot_general(vown[sel].reshape(part * nj, nk), mat_own, contract, preferred_element_type=F32)
            term += lax.dot_general(vpar[sel].reshape(part * nj, nk), mat_par, contract, preferred_element_type=F32)
            term = term.astype(BF16).astype(F32).reshape(part, nj, LANES)
            acc = v1[sel].astype(F32) + v2[sel].astype(F32) + term
            if stage == 0:
                vw[sel] = (vd[sel] * acc.astype(BF16).astype(F32)).astype(BF16)
            else:
                vz[sel] = acc

        if stage == 0:
            store = pltpu.make_async_copy(vw, w.at[c], store_sem.at[0])
        else:
            store = pltpu.make_async_copy(vz, z_ref.at[r, :, :, aligned(half, LANES)], store_sem.at[0])
        store.start()
        store.wait()

    for stage in range(2):
        if stage == 0:
            @pl.loop(0, chunks)
            def _(c):
                start_out(0, c)

        @pl.loop(0, chunks)
        def _(c):
            product_one(stage, c)
            product_two(stage, c)

        @pl.loop(0, chunks)
        def _(c):
            out_c(stage, c).wait_recv()

        @pl.loop(0, chunks)
        def _(c):
            total(stage, c)
            if stage == 0:
                start_out(1, c)

    for stage in range(2):
        @pl.loop(0, chunks)
        def _(c):
            for n in range(n1 - 1):
                out_y(stage, c, n).wait_send()
                back_y(stage, c, n).wait_send()
            for n in range(n2 - 1):
                out_x(stage, c, n).wait_send()
                back_x(stage, c, n).wait_send()
            out_c(stage, c).wait_send()


def solution(mesh):
    n1, n2, n3 = mesh.shape['mode1'], mesh.shape['mode2'], mesh.shape['mode3']
    vol_spec = P('rhs', 'mode1', 'mode2', 'mode3')
    diag_spec = P('mode1', 'mode2', 'mode3')

    def local_op(x_vol, diag_vals, *mats):
        rhs, ni, nj, nk = x_vol.shape
        dims = (n1, n2, n3, rhs, ni, nj, nk)
        halves = nk // LANES
        chunks = rhs * halves
        steps = 2 * chunks
        jc, ic = nj // n1, ni // n2
        hbm = pl.BlockSpec(memory_space=pltpu.HBM)
        vmem = pl.BlockSpec(memory_space=pltpu.VMEM)
        dma = pltpu.SemaphoreType.DMA
        block = (ni, nj, LANES)
        outs = [
            jax.ShapeDtypeStruct(x_vol.shape, F32),
            jax.ShapeDtypeStruct((steps, n1 * ni, jc, LANES), BF16),
            jax.ShapeDtypeStruct((steps, ic, n2 * nj, LANES), BF16),
            jax.ShapeDtypeStruct((steps,) + block, BF16),
            jax.ShapeDtypeStruct((steps, n1 * ni, jc, LANES), BF16),
            jax.ShapeDtypeStruct((steps, ic, n2 * nj, LANES), BF16),
            jax.ShapeDtypeStruct((steps,) + block, BF16),
            jax.ShapeDtypeStruct((steps,) + block, BF16),
            jax.ShapeDtypeStruct((chunks,) + block, BF16),
        ]
        scratch = [
            pltpu.VMEM((n1 * ni, jc, LANES), BF16),
            pltpu.VMEM((n1 * ni * jc, LANES), F32),
            pltpu.VMEM((n1 * ni, jc, LANES), BF16),
            pltpu.VMEM((ic, n2 * nj, LANES), BF16),
            pltpu.VMEM((ic, n2 * nj, LANES), BF16),
            pltpu.VMEM(block, BF16),
            pltpu.VMEM(block, BF16),
            pltpu.VMEM((ni, nj, nk), BF16),
            pltpu.VMEM((ni, nj, nk), BF16),
            pltpu.VMEM(block, F32),
            pltpu.VMEM(block, BF16),
            pltpu.VMEM(block, F32),
            dma((steps, n1 - 1)), dma((steps, n1 - 1)),
            dma((steps, n2 - 1)), dma((steps, n2 - 1)),
            dma((steps,)), dma((steps,)),
            dma((steps, n1 - 1)), dma((steps, n1 - 1)),
            dma((steps, n2 - 1)), dma((steps, n2 - 1)),
            dma((3 + 2 * halves,)), dma((max(n1, n2),)),
        ]
        return pl.pallas_call(
            functools.partial(kernel, dims),
            out_shape=outs,
            in_specs=[hbm, hbm] + [vmem] * 6,
            out_specs=[hbm] * len(outs),
            scratch_shapes=scratch,
            compiler_params=pltpu.CompilerParams(collective_id=0, has_side_effects=True, vmem_limit_bytes=56 * 2 ** 20),
        )(x_vol, diag_vals, *mats)[0]

    return jax.shard_map(local_op, mesh=mesh, in_specs=(vol_spec, diag_spec, P(), P(), P(), P(), P(), P()), out_specs=vol_spec, check_vma=False)
```

```python
import functools

import jax
import jax.numpy as jnp
from jax import lax
from jax.experimental import pallas as pl
from jax.experimental.pallas import tpu as pltpu
from jax.sharding import PartitionSpec as P

MESH = pl.DeviceIdType.MESH
F32, BF16 = jnp.float32, jnp.bfloat16
LANES = 128


def aligned(index, size):
    return pl.ds(pl.multiple_of(index * size, size), size)


def kernel(dims, x_ref, d_ref, a1_ref, a2_ref, a3_ref, b1_ref, b2_ref, b3_ref,
           z_ref, lin1, lin2, lin3, out1, out2, t1, t2, w,
           ma1, ma2, ma3, mb1, mb2, mb3,
           vin1, vscr, vout1, vin2, vout2, v1, v2, vown, vpar, vd, vw, last1, last2,
           y_send, y_recv, x_send, x_recv, c_send, c_recv,
           y_send2, y_recv2, x_send2, x_recv2, mat_sem, load_sem, store_sem):
    n1, n2, n3, rhs, ni, nj, nk = dims
    halves = nk // LANES
    chunks = rhs * halves
    jc, ic = nj // n1, ni // n2
    me1, me2, me3 = lax.axis_index('mode1'), lax.axis_index('mode2'), lax.axis_index('mode3')
    peer1 = [lax.rem(me1 + s, n1) for s in range(1, n1)]
    peer2 = [lax.rem(me2 + s, n2) for s in range(1, n2)]
    peer3 = lax.rem(me3 + 1, n3)

    barrier = pltpu.get_barrier_semaphore()
    for axis, peers in (('mode1', peer1), ('mode2', peer2), ('mode3', [peer3])):
        for peer in peers:
            pl.semaphore_signal(barrier, inc=1, device_id={axis: peer}, device_id_type=MESH)
    pl.semaphore_wait(barrier, n1 + n2 + n3 - 3)

    def remote(src, dst, send, recv, axis, peer):
        return pltpu.make_async_remote_copy(src_ref=src, dst_ref=dst, send_sem=send, recv_sem=recv,
                                            device_id={axis: peer}, device_id_type=MESH)

    def field(stage, c):
        if stage == 0:
            return x_ref.at[c // halves, :, :, aligned(lax.rem(c, halves), LANES)]
        return w.at[c]

    def out_y(stage, c, n):
        g = stage * chunks + c
        return remote(field(stage, c).at[:, aligned(peer1[n], jc), :], lin1.at[g, aligned(me1, ni)],
                      y_send.at[g, n], y_recv.at[g, n], 'mode1', peer1[n])

    def out_x(stage, c, n):
        g = stage * chunks + c
        return remote(field(stage, c).at[aligned(peer2[n], ic)], lin2.at[g, :, aligned(me2, nj), :],
                      x_send.at[g, n], x_recv.at[g, n], 'mode2', peer2[n])

    def out_c(stage, c):
        g = stage * chunks + c
        return remote(field(stage, c), lin3.at[g], c_send.at[g], c_recv.at[g], 'mode3', peer3)

    def is_last(stage, c):
        return stage == 1 and isinstance(c, int) and c == chunks - 1

    def back_y(stage, c, n):
        g = stage * chunks + c
        dst = last1 if is_last(stage, c) else t1.at[g]
        return remote(out1.at[g, aligned(peer1[n], ni)], dst.at[:, aligned(me1, jc), :],
                      y_send2.at[g, n], y_recv2.at[g, n], 'mode1', peer1[n])

    def back_x(stage, c, n):
        g = stage * chunks + c
        dst = last2 if is_last(stage, c) else t2.at[g]
        return remote(out2.at[g, :, aligned(peer2[n], nj), :], dst.at[aligned(me2, ic)],
                      x_send2.at[g, n], x_recv2.at[g, n], 'mode2', peer2[n])

    order1 = sorted(range(n1 - 1), key=lambda n: min(n + 1, n1 - n - 1))
    order2 = sorted(range(n2 - 1), key=lambda n: min(n + 1, n2 - n - 1))

    def start_out(stage, c):
        for n in order1:
            out_y(stage, c, n).start()
        for n in order2:
            out_x(stage, c, n).start()
        out_c(stage, c).start()

    def product_one(stage, c):
        g = stage * chunks + c
        mat = (ma1, mb1)[stage]
        for n in range(n1 - 1):
            out_y(stage, c, n).wait_recv()
        loads = [pltpu.make_async_copy(field(stage, c).at[:, aligned(me1, jc), :], vin1.at[aligned(me1, ni)], load_sem.at[0])]
        loads += [pltpu.make_async_copy(lin1.at[g, aligned(peer1[n], ni)], vin1.at[aligned(peer1[n], ni)], load_sem.at[n + 1])
                  for n in range(n1 - 1)]
        for copy in loads:
            copy.start()
        for copy in loads:
            copy.wait()
        full = n1 * ni
        part = 32

        @pl.loop(0, full // part)
        def _(b):
            vscr[pl.ds(pl.multiple_of(b * part * jc, part * jc), part * jc), :] = (
                vin1[pl.ds(b * part, part)].astype(F32).reshape(part * jc, LANES))

        @pl.loop(0, jc // 2)
        def _(b):
            rows = [pl.ds(2 * b + h, full, stride=jc) for h in range(2)]
            rhs_mat = jnp.concatenate([vscr[row, :].astype(BF16) for row in rows], axis=1)
            res = jnp.dot(mat[...], rhs_mat, preferred_element_type=F32)
            for h in range(2):
                vscr[rows[h], :] = res[:, h * LANES:(h + 1) * LANES]

        @pl.loop(0, full // part)
        def _(b):
            vout1[pl.ds(b * part, part)] = (
                vscr[pl.ds(pl.multiple_of(b * part * jc, part * jc), part * jc), :].reshape(part, jc, LANES).astype(BF16))

        stores = [pltpu.make_async_copy(vout1.at[aligned(peer1[n], ni)], out1.at[g, aligned(peer1[n], ni)], store_sem.at[n + 1])
                  for n in range(n1 - 1)]
        if not is_last(stage, c):
            stores += [pltpu.make_async_copy(vout1.at[aligned(me1, ni)], t1.at[g, :, aligned(me1, jc), :], store_sem.at[0])]
        for copy in stores:
            copy.start()
        for copy in stores:
            copy.wait()
        for n in order1:
            back_y(stage, c, n).start()

    def product_two(stage, c):
        g = stage * chunks + c
        mat = (ma2, mb2)[stage]
        for n in range(n2 - 1):
            out_x(stage, c, n).wait_recv()
        loads = [pltpu.make_async_copy(field(stage, c).at[aligned(me2, ic)], vin2.at[:, aligned(me2, nj), :], load_sem.at[0])]
        loads += [pltpu.make_async_copy(lin2.at[g, :, aligned(peer2[n], nj), :], vin2.at[:, aligned(peer2[n], nj), :], load_sem.at[n + 1])
                  for n in range(n2 - 1)]
        for copy in loads:
            copy.start()
        for copy in loads:
            copy.wait()

        @pl.loop(0, ic // 2)
        def _(b):
            rhs_mat = jnp.concatenate([vin2[2 * b], vin2[2 * b + 1]], axis=1)
            res = jnp.dot(mat[...], rhs_mat, preferred_element_type=F32).astype(BF16)
            vout2[2 * b] = res[:, :LANES]
            vout2[2 * b + 1] = res[:, LANES:]

        stores = [pltpu.make_async_copy(vout2.at[:, aligned(peer2[n], nj), :], out2.at[g, :, aligned(peer2[n], nj), :], store_sem.at[n + 1])
                  for n in range(n2 - 1)]
        if not is_last(stage, c):
            stores += [pltpu.make_async_copy(vout2.at[:, aligned(me2, nj), :], t2.at[g, aligned(me2, ic)], store_sem.at[0])]
        for copy in stores:
            copy.start()
        for copy in stores:
            copy.wait()
        for n in order2:
            back_x(stage, c, n).start()

    def wait_back(stage, c):
        for n in range(n1 - 1):
            back_y(stage, c, n).wait_recv()
        for n in range(n2 - 1):
            back_x(stage, c, n).wait_recv()

    def third(stage, c, put):
        r, half = c // halves, lax.rem(c, halves)
        mat = (ma3, mb3)[stage]
        rows = pl.ds(pl.multiple_of(me3 * nk + half * LANES, LANES), LANES)
        mat_own = mat[rows, aligned(me3, nk)]
        mat_par = mat[rows, aligned(peer3, nk)]
        contract = (((1,), (1,)), ((), ()))
        part = 8

        @pl.loop(0, ni // part)
        def _(b):
            sel = pl.ds(b * part, part)
            term = lax.dot_general(vown[sel].reshape(part * nj, nk), mat_own, contract, preferred_element_type=F32)
            term += lax.dot_general(vpar[sel].reshape(part * nj, nk), mat_par, contract, preferred_element_type=F32)
            put(sel, term.astype(BF16).astype(F32).reshape(part, nj, LANES))

    def run(copies):
        for copy in copies:
            copy.start()
        for copy in copies:
            copy.wait()

    def load_field(stage, c):
        r = c // halves
        loads = []
        for h in range(halves):
            lanes = pl.ds(h * LANES, LANES)
            loads += [pltpu.make_async_copy(field(stage, r * halves + h), vown.at[:, :, lanes], load_sem.at[2 + h]),
                      pltpu.make_async_copy(lin3.at[stage * chunks + r * halves + h], vpar.at[:, :, lanes], load_sem.at[2 + halves + h])]
        return loads

    def load_terms(stage, c):
        g = stage * chunks + c
        return [pltpu.make_async_copy(t1.at[g], v1, load_sem.at[0]), pltpu.make_async_copy(t2.at[g], v2, load_sem.at[1])]

    def total_a(c):
        half = lax.rem(c, halves)
        wait_back(0, c)
        run(load_terms(0, c) + load_field(0, c)
            + [pltpu.make_async_copy(d_ref.at[:, :, aligned(half, LANES)], vd, load_sem.at[2 + 2 * halves])])

        def put(sel, term):
            acc = v1[sel].astype(F32) + v2[sel].astype(F32) + term
            vw[sel] = (vd[sel] * acc.astype(BF16).astype(F32)).astype(BF16)

        third(0, c, put)
        run([pltpu.make_async_copy(vw, w.at[c], store_sem.at[0])])

    def total_b(c):
        r, lanes = c // halves, aligned(lax.rem(c, halves), LANES)
        run(load_field(1, c))

        def put(sel, term):
            z_ref[r, sel, :, lanes] = term

        third(1, c, put)

        def add(block, rows, cols, part):
            start, count = rows

            @pl.loop(0, count // part)
            def _(b):
                sel = pl.ds(start + b * part, part)
                z_ref[r, sel, cols, lanes] = block(b * part, part) + z_ref[r, sel, cols, lanes]

        if not is_last(1, c):
            wait_back(1, c)
            run(load_terms(1, c))
            add(lambda i, p: v1[pl.ds(i, p)].astype(F32) + v2[pl.ds(i, p)].astype(F32), (0, ni), slice(None), 8)
            return
        add(lambda i, p: vout1[pl.ds(me1 * ni + i, p)].astype(F32), (0, ni), aligned(me1, jc), 8)
        add(lambda i, p: vout2[pl.ds(i, p), aligned(me2, nj), :].astype(F32), (me2 * ic, ic), slice(None), 8)
        for m in range(max(n1, n2) - 1):
            if m < n1 - 1:
                peer = peer1[n1 - 2 - order1[m]]
                back_y(1, c, order1[m]).wait_recv()
                add(lambda i, p: last1[pl.ds(i, p), aligned(peer, jc), :].astype(F32), (0, ni), aligned(peer, jc), 8)
            if m < n2 - 1:
                peer = peer2[n2 - 2 - order2[m]]
                back_x(1, c, order2[m]).wait_recv()
                add(lambda i, p: last2[pl.ds(peer * ic + i, p)].astype(F32), (peer * ic, ic), slice(None), 8)

    @pl.loop(0, chunks)
    def _(c):
        start_out(0, c)

    run([pltpu.make_async_copy(src, dst, mat_sem.at[m]) for m, (src, dst) in enumerate(
        zip((a1_ref, a2_ref, a3_ref, b1_ref, b2_ref, b3_ref), (ma1, ma2, ma3, mb1, mb2, mb3)))])

    @pl.loop(0, chunks)
    def _(c):
        product_one(0, c)
        product_two(0, c)

    @pl.loop(0, chunks)
    def _(c):
        out_c(0, c).wait_recv()

    @pl.loop(0, chunks)
    def _(c):
        total_a(c)
        start_out(1, c)

    @pl.loop(0, chunks - 1)
    def _(c):
        product_one(1, c)
        product_two(1, c)

    product_one(1, chunks - 1)
    product_two(1, chunks - 1)

    @pl.loop(0, chunks)
    def _(c):
        out_c(1, c).wait_recv()

    @pl.loop(0, chunks - 1)
    def _(c):
        total_b(c)

    total_b(chunks - 1)

    for stage in range(2):
        @pl.loop(0, chunks)
        def _(c):
            for n in range(n1 - 1):
                out_y(stage, c, n).wait_send()
                back_y(stage, c, n).wait_send()
            for n in range(n2 - 1):
                out_x(stage, c, n).wait_send()
                back_x(stage, c, n).wait_send()
            out_c(stage, c).wait_send()


def solution(mesh):
    n1, n2, n3 = mesh.shape['mode1'], mesh.shape['mode2'], mesh.shape['mode3']
    vol_spec = P('rhs', 'mode1', 'mode2', 'mode3')
    diag_spec = P('mode1', 'mode2', 'mode3')

    def local_op(x_vol, diag_vals, *mats):
        rhs, ni, nj, nk = x_vol.shape
        dims = (n1, n2, n3, rhs, ni, nj, nk)
        halves = nk // LANES
        chunks = rhs * halves
        steps = 2 * chunks
        jc, ic = nj // n1, ni // n2
        hbm = pl.BlockSpec(memory_space=pltpu.HBM)
        vmem = pl.BlockSpec(memory_space=pltpu.VMEM)
        dma = pltpu.SemaphoreType.DMA
        block = (ni, nj, LANES)
        outs = [
            pltpu.VMEM(x_vol.shape, F32),
            jax.ShapeDtypeStruct((steps, n1 * ni, jc, LANES), BF16),
            jax.ShapeDtypeStruct((steps, ic, n2 * nj, LANES), BF16),
            jax.ShapeDtypeStruct((steps,) + block, BF16),
            jax.ShapeDtypeStruct((steps, n1 * ni, jc, LANES), BF16),
            jax.ShapeDtypeStruct((steps, ic, n2 * nj, LANES), BF16),
            jax.ShapeDtypeStruct((steps,) + block, BF16),
            jax.ShapeDtypeStruct((steps,) + block, BF16),
            jax.ShapeDtypeStruct((chunks,) + block, BF16),
        ]
        scratch = [pltpu.VMEM(mat.shape, mat.dtype) for mat in mats] + [
            pltpu.VMEM((n1 * ni, jc, LANES), BF16),
            pltpu.VMEM((n1 * ni * jc, LANES), F32),
            pltpu.VMEM((n1 * ni, jc, LANES), BF16),
            pltpu.VMEM((ic, n2 * nj, LANES), BF16),
            pltpu.VMEM((ic, n2 * nj, LANES), BF16),
            pltpu.VMEM(block, BF16),
            pltpu.VMEM(block, BF16),
            pltpu.VMEM((ni, nj, nk), BF16),
            pltpu.VMEM((ni, nj, nk), BF16),
            pltpu.VMEM(block, F32),
            pltpu.VMEM(block, BF16),
            pltpu.VMEM(block, BF16),
            pltpu.VMEM(block, BF16),
            dma((steps, n1 - 1)), dma((steps, n1 - 1)),
            dma((steps, n2 - 1)), dma((steps, n2 - 1)),
            dma((steps,)), dma((steps,)),
            dma((steps, n1 - 1)), dma((steps, n1 - 1)),
            dma((steps, n2 - 1)), dma((steps, n2 - 1)),
            dma((len(mats),)), dma((max(3 + 2 * halves, n1, n2),)), dma((max(n1, n2),)),
        ]
        return pl.pallas_call(
            functools.partial(kernel, dims),
            out_shape=outs,
            in_specs=[hbm] * (2 + len(mats)),
            out_specs=[vmem] + [hbm] * (len(outs) - 1),
            scratch_shapes=scratch,
            compiler_params=pltpu.CompilerParams(collective_id=0, has_side_effects=True, vmem_limit_bytes=46 * 2 ** 20),
        )(x_vol, diag_vals, *mats)[0]

    return jax.shard_map(local_op, mesh=mesh, in_specs=(vol_spec, diag_spec, P(), P(), P(), P(), P(), P()), out_specs=vol_spec, check_vma=False)
```

```python
import functools

import jax
import jax.numpy as jnp
from jax import lax
from jax.experimental import pallas as pl
from jax.experimental.pallas import tpu as pltpu
from jax.sharding import PartitionSpec as P

MESH = pl.DeviceIdType.MESH
F32, BF16 = jnp.float32, jnp.bfloat16
LANES = 128


def aligned(index, size):
    return pl.ds(pl.multiple_of(index * size, size), size)


def kernel(dims, x_ref, d_ref, a1_ref, a2_ref, a3_ref, b1_ref, b2_ref, b3_ref,
           z_ref, lin1, lin2, lin3, out1, out2, t1, t2, w,
           ma1, ma2, ma3, mb1, mb2, mb3,
           vin1, vscr, vout1, vin2, vout2, v1, v2, vown, vpar, vd, vw, last1, last2,
           y_send, y_recv, x_send, x_recv, c_send, c_recv,
           y_send2, y_recv2, x_send2, x_recv2, mat_sem, load_sem, store_sem):
    n1, n2, n3, rhs, ni, nj, nk = dims
    halves = nk // LANES
    chunks = rhs * halves
    jc, ic = nj // n1, ni // n2
    me1, me2, me3 = lax.axis_index('mode1'), lax.axis_index('mode2'), lax.axis_index('mode3')
    peer1 = [lax.rem(me1 + s, n1) for s in range(1, n1)]
    peer2 = [lax.rem(me2 + s, n2) for s in range(1, n2)]
    peer3 = lax.rem(me3 + 1, n3)

    barrier = pltpu.get_barrier_semaphore()
    for axis, peers in (('mode1', peer1), ('mode2', peer2), ('mode3', [peer3])):
        for peer in peers:
            pl.semaphore_signal(barrier, inc=1, device_id={axis: peer}, device_id_type=MESH)
    pl.semaphore_wait(barrier, n1 + n2 + n3 - 3)

    def remote(src, dst, send, recv, axis, peer):
        return pltpu.make_async_remote_copy(src_ref=src, dst_ref=dst, send_sem=send, recv_sem=recv,
                                            device_id={axis: peer}, device_id_type=MESH)

    def field(stage, c):
        if stage == 0:
            return x_ref.at[c // halves, :, :, aligned(lax.rem(c, halves), LANES)]
        return w.at[c]

    def out_y(stage, c, n):
        g = stage * chunks + c
        return remote(field(stage, c).at[:, aligned(peer1[n], jc), :], lin1.at[g, aligned(me1, ni)],
                      y_send.at[g, n], y_recv.at[g, n], 'mode1', peer1[n])

    def out_x(stage, c, n):
        g = stage * chunks + c
        return remote(field(stage, c).at[aligned(peer2[n], ic)], lin2.at[g, :, aligned(me2, nj), :],
                      x_send.at[g, n], x_recv.at[g, n], 'mode2', peer2[n])

    def out_c(stage, c):
        g = stage * chunks + c
        return remote(field(stage, c), lin3.at[g], c_send.at[g], c_recv.at[g], 'mode3', peer3)

    def is_last(stage, c):
        return stage == 1 and isinstance(c, int) and c == chunks - 1

    def back_y(stage, c, n):
        g = stage * chunks + c
        dst = last1 if is_last(stage, c) else t1.at[g]
        return remote(out1.at[g, aligned(peer1[n], ni)], dst.at[:, aligned(me1, jc), :],
                      y_send2.at[g, n], y_recv2.at[g, n], 'mode1', peer1[n])

    def back_x(stage, c, n):
        g = stage * chunks + c
        dst = last2 if is_last(stage, c) else t2.at[g]
        return remote(out2.at[g, :, aligned(peer2[n], nj), :], dst.at[aligned(me2, ic)],
                      x_send2.at[g, n], x_recv2.at[g, n], 'mode2', peer2[n])

    order1 = sorted(range(n1 - 1), key=lambda n: min(n + 1, n1 - n - 1))
    order2 = sorted(range(n2 - 1), key=lambda n: min(n + 1, n2 - n - 1))

    def start_out(stage, c):
        for n in order1:
            out_y(stage, c, n).start()
        for n in order2:
            out_x(stage, c, n).start()
        out_c(stage, c).start()

    def product_one(stage, c):
        g = stage * chunks + c
        mat = (ma1, mb1)[stage]
        for n in range(n1 - 1):
            out_y(stage, c, n).wait_recv()
        loads = [pltpu.make_async_copy(field(stage, c).at[:, aligned(me1, jc), :], vin1.at[aligned(me1, ni)], load_sem.at[0])]
        loads += [pltpu.make_async_copy(lin1.at[g, aligned(peer1[n], ni)], vin1.at[aligned(peer1[n], ni)], load_sem.at[n + 1])
                  for n in range(n1 - 1)]
        for copy in loads:
            copy.start()
        for copy in loads:
            copy.wait()
        full = n1 * ni
        part = 32

        @pl.loop(0, full // part)
        def _(b):
            vscr[pl.ds(pl.multiple_of(b * part * jc, part * jc), part * jc), :] = (
                vin1[pl.ds(b * part, part)].astype(F32).reshape(part * jc, LANES))

        @pl.loop(0, jc // 2)
        def _(b):
            rows = [pl.ds(2 * b + h, full, stride=jc) for h in range(2)]
            rhs_mat = jnp.concatenate([vscr[row, :].astype(BF16) for row in rows], axis=1)
            res = jnp.dot(mat[...], rhs_mat, preferred_element_type=F32)
            for h in range(2):
                vscr[rows[h], :] = res[:, h * LANES:(h + 1) * LANES]

        @pl.loop(0, full // part)
        def _(b):
            vout1[pl.ds(b * part, part)] = (
                vscr[pl.ds(pl.multiple_of(b * part * jc, part * jc), part * jc), :].reshape(part, jc, LANES).astype(BF16))

        stores = [pltpu.make_async_copy(vout1.at[aligned(peer1[n], ni)], out1.at[g, aligned(peer1[n], ni)], store_sem.at[n + 1])
                  for n in range(n1 - 1)]
        if not is_last(stage, c):
            stores += [pltpu.make_async_copy(vout1.at[aligned(me1, ni)], t1.at[g, :, aligned(me1, jc), :], store_sem.at[0])]
        for copy in stores:
            copy.start()
        for copy in stores:
            copy.wait()
        for n in order1:
            back_y(stage, c, n).start()

    def product_two(stage, c):
        g = stage * chunks + c
        mat = (ma2, mb2)[stage]
        for n in range(n2 - 1):
            out_x(stage, c, n).wait_recv()
        loads = [pltpu.make_async_copy(field(stage, c).at[aligned(me2, ic)], vin2.at[:, aligned(me2, nj), :], load_sem.at[0])]
        loads += [pltpu.make_async_copy(lin2.at[g, :, aligned(peer2[n], nj), :], vin2.at[:, aligned(peer2[n], nj), :], load_sem.at[n + 1])
                  for n in range(n2 - 1)]
        for copy in loads:
            copy.start()
        for copy in loads:
            copy.wait()

        @pl.loop(0, ic // 2)
        def _(b):
            rhs_mat = jnp.concatenate([vin2[2 * b], vin2[2 * b + 1]], axis=1)
            res = jnp.dot(mat[...], rhs_mat, preferred_element_type=F32).astype(BF16)
            vout2[2 * b] = res[:, :LANES]
            vout2[2 * b + 1] = res[:, LANES:]

        stores = [pltpu.make_async_copy(vout2.at[:, aligned(peer2[n], nj), :], out2.at[g, :, aligned(peer2[n], nj), :], store_sem.at[n + 1])
                  for n in range(n2 - 1)]
        if not is_last(stage, c):
            stores += [pltpu.make_async_copy(vout2.at[:, aligned(me2, nj), :], t2.at[g, aligned(me2, ic)], store_sem.at[0])]
        for copy in stores:
            copy.start()
        for copy in stores:
            copy.wait()
        for n in order2:
            back_x(stage, c, n).start()

    def wait_back(stage, c):
        for n in range(n1 - 1):
            back_y(stage, c, n).wait_recv()
        for n in range(n2 - 1):
            back_x(stage, c, n).wait_recv()

    def third(stage, c, put):
        r, half = c // halves, lax.rem(c, halves)
        mat = (ma3, mb3)[stage]
        rows = pl.ds(pl.multiple_of(me3 * nk + half * LANES, LANES), LANES)
        mat_own = mat[rows, aligned(me3, nk)]
        mat_par = mat[rows, aligned(peer3, nk)]
        contract = (((1,), (1,)), ((), ()))
        part = 8

        @pl.loop(0, ni // part)
        def _(b):
            sel = pl.ds(b * part, part)
            term = lax.dot_general(vown[sel].reshape(part * nj, nk), mat_own, contract, preferred_element_type=F32)
            term += lax.dot_general(vpar[sel].reshape(part * nj, nk), mat_par, contract, preferred_element_type=F32)
            put(sel, term.astype(BF16).astype(F32).reshape(part, nj, LANES))

    def run(copies):
        for copy in copies:
            copy.start()
        for copy in copies:
            copy.wait()

    def load_field(stage, c):
        r = c // halves
        loads = []
        for h in range(halves):
            lanes = pl.ds(h * LANES, LANES)
            loads += [pltpu.make_async_copy(field(stage, r * halves + h), vown.at[:, :, lanes], load_sem.at[2 + h]),
                      pltpu.make_async_copy(lin3.at[stage * chunks + r * halves + h], vpar.at[:, :, lanes], load_sem.at[2 + halves + h])]
        return loads

    def load_terms(stage, c):
        g = stage * chunks + c
        return [pltpu.make_async_copy(t1.at[g], v1, load_sem.at[0]), pltpu.make_async_copy(t2.at[g], v2, load_sem.at[1])]

    def total_a(c):
        half = lax.rem(c, halves)
        wait_back(0, c)
        run(load_terms(0, c) + load_field(0, c)
            + [pltpu.make_async_copy(d_ref.at[:, :, aligned(half, LANES)], vd, load_sem.at[2 + 2 * halves])])

        def put(sel, term):
            acc = v1[sel].astype(F32) + v2[sel].astype(F32) + term
            vw[sel] = (vd[sel] * acc.astype(BF16).astype(F32)).astype(BF16)

        third(0, c, put)
        run([pltpu.make_async_copy(vw, w.at[c], store_sem.at[0])])

    def wait_out_sends(stage, c):
        for n in range(n1 - 1):
            out_y(stage, c, n).wait_send()
        for n in range(n2 - 1):
            out_x(stage, c, n).wait_send()
        out_c(stage, c).wait_send()

    def wait_back_sends(stage, c):
        for n in range(n1 - 1):
            back_y(stage, c, n).wait_send()
        for n in range(n2 - 1):
            back_x(stage, c, n).wait_send()

    def total_b(c):
        r, lanes = c // halves, aligned(lax.rem(c, halves), LANES)
        run(load_field(1, c))

        def put(sel, term):
            z_ref[r, sel, :, lanes] = term

        third(1, c, put)

        def add(block, rows, cols, part):
            start, count = rows

            @pl.loop(0, count // part)
            def _(b):
                sel = pl.ds(start + b * part, part)
                z_ref[r, sel, cols, lanes] = block(b * part, part) + z_ref[r, sel, cols, lanes]

        if not is_last(1, c):
            wait_back(1, c)
            run(load_terms(1, c))
            add(lambda i, p: v1[pl.ds(i, p)].astype(F32) + v2[pl.ds(i, p)].astype(F32), (0, ni), slice(None), 8)
            return
        add(lambda i, p: vout1[pl.ds(me1 * ni + i, p)].astype(F32), (0, ni), aligned(me1, jc), 8)
        add(lambda i, p: vout2[pl.ds(i, p), aligned(me2, nj), :].astype(F32), (me2 * ic, ic), slice(None), 8)
        @pl.loop(0, chunks)
        def _(e):
            wait_out_sends(0, e)
            wait_back_sends(0, e)
            wait_out_sends(1, e)

        @pl.loop(0, chunks - 1)
        def _(e):
            wait_back_sends(1, e)

        for m in range(max(n1, n2) - 1):
            if m < n1 - 1:
                peer = peer1[n1 - 2 - order1[m]]
                back_y(1, c, order1[m]).wait_recv()
                add(lambda i, p: last1[pl.ds(i, p), aligned(peer, jc), :].astype(F32), (0, ni), aligned(peer, jc), 8)
            if m < n2 - 1:
                peer = peer2[n2 - 2 - order2[m]]
                back_x(1, c, order2[m]).wait_recv()
                add(lambda i, p: last2[pl.ds(peer * ic + i, p)].astype(F32), (peer * ic, ic), slice(None), 8)

    @pl.loop(0, chunks)
    def _(c):
        start_out(0, c)

    run([pltpu.make_async_copy(src, dst, mat_sem.at[m]) for m, (src, dst) in enumerate(
        zip((a1_ref, a2_ref, a3_ref, b1_ref, b2_ref, b3_ref), (ma1, ma2, ma3, mb1, mb2, mb3)))])

    @pl.loop(0, chunks)
    def _(c):
        product_one(0, c)
        product_two(0, c)

    @pl.loop(0, chunks)
    def _(c):
        out_c(0, c).wait_recv()

    @pl.loop(0, chunks)
    def _(c):
        total_a(c)
        start_out(1, c)

    @pl.loop(0, chunks - 1)
    def _(c):
        product_one(1, c)
        product_two(1, c)

    product_one(1, chunks - 1)
    product_two(1, chunks - 1)

    @pl.loop(0, chunks)
    def _(c):
        out_c(1, c).wait_recv()

    @pl.loop(0, chunks - 1)
    def _(c):
        total_b(c)

    total_b(chunks - 1)
    wait_back_sends(1, chunks - 1)


def solution(mesh):
    n1, n2, n3 = mesh.shape['mode1'], mesh.shape['mode2'], mesh.shape['mode3']
    vol_spec = P('rhs', 'mode1', 'mode2', 'mode3')
    diag_spec = P('mode1', 'mode2', 'mode3')

    def local_op(x_vol, diag_vals, *mats):
        rhs, ni, nj, nk = x_vol.shape
        dims = (n1, n2, n3, rhs, ni, nj, nk)
        halves = nk // LANES
        chunks = rhs * halves
        steps = 2 * chunks
        jc, ic = nj // n1, ni // n2
        hbm = pl.BlockSpec(memory_space=pltpu.HBM)
        vmem = pl.BlockSpec(memory_space=pltpu.VMEM)
        dma = pltpu.SemaphoreType.DMA
        block = (ni, nj, LANES)
        outs = [
            pltpu.VMEM(x_vol.shape, F32),
            jax.ShapeDtypeStruct((steps, n1 * ni, jc, LANES), BF16),
            jax.ShapeDtypeStruct((steps, ic, n2 * nj, LANES), BF16),
            jax.ShapeDtypeStruct((steps,) + block, BF16),
            jax.ShapeDtypeStruct((steps, n1 * ni, jc, LANES), BF16),
            jax.ShapeDtypeStruct((steps, ic, n2 * nj, LANES), BF16),
            jax.ShapeDtypeStruct((steps,) + block, BF16),
            jax.ShapeDtypeStruct((steps,) + block, BF16),
            jax.ShapeDtypeStruct((chunks,) + block, BF16),
        ]
        scratch = [pltpu.VMEM(mat.shape, mat.dtype) for mat in mats] + [
            pltpu.VMEM((n1 * ni, jc, LANES), BF16),
            pltpu.VMEM((n1 * ni * jc, LANES), F32),
            pltpu.VMEM((n1 * ni, jc, LANES), BF16),
            pltpu.VMEM((ic, n2 * nj, LANES), BF16),
            pltpu.VMEM((ic, n2 * nj, LANES), BF16),
            pltpu.VMEM(block, BF16),
            pltpu.VMEM(block, BF16),
            pltpu.VMEM((ni, nj, nk), BF16),
            pltpu.VMEM((ni, nj, nk), BF16),
            pltpu.VMEM(block, F32),
            pltpu.VMEM(block, BF16),
            pltpu.VMEM(block, BF16),
            pltpu.VMEM(block, BF16),
            dma((steps, n1 - 1)), dma((steps, n1 - 1)),
            dma((steps, n2 - 1)), dma((steps, n2 - 1)),
            dma((steps,)), dma((steps,)),
            dma((steps, n1 - 1)), dma((steps, n1 - 1)),
            dma((steps, n2 - 1)), dma((steps, n2 - 1)),
            dma((len(mats),)), dma((max(3 + 2 * halves, n1, n2),)), dma((max(n1, n2),)),
        ]
        res = pl.pallas_call(
            functools.partial(kernel, dims),
            out_shape=outs,
            in_specs=[hbm] * (2 + len(mats)),
            out_specs=[vmem] + [hbm] * (len(outs) - 1),
            scratch_shapes=scratch,
            compiler_params=pltpu.CompilerParams(collective_id=0, has_side_effects=True, vmem_limit_bytes=46 * 2 ** 20),
        )(x_vol, diag_vals, *mats)[0]
        parts = 8

        def put(z_in, z_out, sem):
            copies = [pltpu.make_async_copy(z_in.at[r, pl.ds(b * (ni // parts), ni // parts)], z_out.at[r, pl.ds(b * (ni // parts), ni // parts)], sem.at[r, b])
                      for r in range(rhs) for b in range(parts)]
            for copy in copies:
                copy.start()
            for copy in copies:
                copy.wait()

        return pl.pallas_call(put, out_shape=jax.ShapeDtypeStruct(x_vol.shape, F32), in_specs=[vmem], out_specs=hbm,
                              scratch_shapes=[dma((rhs, parts))], compiler_params=pltpu.CompilerParams(vmem_limit_bytes=24 * 2 ** 20))(res)

    return jax.shard_map(local_op, mesh=mesh, in_specs=(vol_spec, diag_spec, P(), P(), P(), P(), P(), P()), out_specs=vol_spec, check_vma=False)
```

```python
import functools

import jax
import jax.numpy as jnp
from jax import lax
from jax.experimental import pallas as pl
from jax.experimental.pallas import tpu as pltpu
from jax.sharding import PartitionSpec as P

MESH = pl.DeviceIdType.MESH
F32, BF16 = jnp.float32, jnp.bfloat16
LANES = 128


def aligned(index, size):
    return pl.ds(pl.multiple_of(index * size, size), size)


def kernel(dims, x_ref, d_ref, a1_ref, a2_ref, a3_ref, b1_ref, b2_ref, b3_ref,
           z_ref, lin1, lin2, lin3, out1, out2, t1, t2, w,
           ma1, ma2, ma3, mb1, mb2, mb3,
           vin1, vscr, vout1, vin2, vout2, v1, v2, vown, vpar, vd, vw, last1, last2,
           y_send, y_recv, x_send, x_recv, c_send, c_recv,
           y_send2, y_recv2, x_send2, x_recv2, mat_sem, load_sem, store_sem):
    n1, n2, n3, rhs, ni, nj, nk = dims
    halves = nk // LANES
    chunks = rhs * halves
    jc, ic = nj // n1, ni // n2
    me1, me2, me3 = lax.axis_index('mode1'), lax.axis_index('mode2'), lax.axis_index('mode3')
    peer1 = [lax.rem(me1 + s, n1) for s in range(1, n1)]
    peer2 = [lax.rem(me2 + s, n2) for s in range(1, n2)]
    peer3 = lax.rem(me3 + 1, n3)

    barrier = pltpu.get_barrier_semaphore()
    for axis, peers in (('mode1', peer1), ('mode2', peer2), ('mode3', [peer3])):
        for peer in peers:
            pl.semaphore_signal(barrier, inc=1, device_id={axis: peer}, device_id_type=MESH)
    pl.semaphore_wait(barrier, n1 + n2 + n3 - 3)

    order1 = sorted(range(n1 - 1), key=lambda n: min(n + 1, n1 - n - 1))
    order2 = sorted(range(n2 - 1), key=lambda n: min(n + 1, n2 - n - 1))

    def remote(src, dst, send, recv, axis, peer):
        return pltpu.make_async_remote_copy(src_ref=src, dst_ref=dst, send_sem=send, recv_sem=recv,
                                            device_id={axis: peer}, device_id_type=MESH)

    def run(copies):
        for copy in copies:
            copy.start()
        for copy in copies:
            copy.wait()

    def field(stage, r):
        return (x_ref, w)[stage].at[r]

    def out_y(stage, r, n):
        q = stage * rhs + r
        return remote(field(stage, r).at[:, aligned(peer1[n], jc), :], lin1.at[q, aligned(me1, ni)],
                      y_send.at[q, n], y_recv.at[q, n], 'mode1', peer1[n])

    def out_x(stage, r, n):
        q = stage * rhs + r
        return remote(field(stage, r).at[aligned(peer2[n], ic)], lin2.at[q, :, aligned(me2, nj), :],
                      x_send.at[q, n], x_recv.at[q, n], 'mode2', peer2[n])

    def out_c(stage, r):
        q = stage * rhs + r
        return remote(field(stage, r), lin3.at[q], c_send.at[q], c_recv.at[q], 'mode3', peer3)

    def is_last(stage, c):
        return stage == 1 and isinstance(c, int) and c == chunks - 1

    def back_y(stage, c, n):
        g = stage * chunks + c
        dst = last1 if is_last(stage, c) else t1.at[g]
        return remote(out1.at[g, aligned(peer1[n], ni)], dst.at[:, aligned(me1, jc), :],
                      y_send2.at[g, n], y_recv2.at[g, n], 'mode1', peer1[n])

    def back_x(stage, c, n):
        g = stage * chunks + c
        dst = last2 if is_last(stage, c) else t2.at[g]
        return remote(out2.at[g, :, aligned(peer2[n], nj), :], dst.at[aligned(me2, ic)],
                      x_send2.at[g, n], x_recv2.at[g, n], 'mode2', peer2[n])

    def start_out(stage, r):
        for n in order1:
            out_y(stage, r, n).start()
        for n in order2:
            out_x(stage, r, n).start()
        out_c(stage, r).start()

    def wait_out(stage, r):
        for n in range(n1 - 1):
            out_y(stage, r, n).wait_recv()
        for n in range(n2 - 1):
            out_x(stage, r, n).wait_recv()

    def wait_back(stage, c):
        for n in range(n1 - 1):
            back_y(stage, c, n).wait_recv()
        for n in range(n2 - 1):
            back_x(stage, c, n).wait_recv()

    def wait_out_sends(stage, r):
        for n in range(n1 - 1):
            out_y(stage, r, n).wait_send()
        for n in range(n2 - 1):
            out_x(stage, r, n).wait_send()
        out_c(stage, r).wait_send()

    def wait_back_sends(stage, c):
        for n in range(n1 - 1):
            back_y(stage, c, n).wait_send()
        for n in range(n2 - 1):
            back_x(stage, c, n).wait_send()

    def product_one(stage, r, h, c):
        q, g, lanes = stage * rhs + r, stage * chunks + c, aligned(h, LANES)
        mat = (ma1, mb1)[stage]
        run([pltpu.make_async_copy(field(stage, r).at[:, aligned(me1, jc), lanes], vin1.at[aligned(me1, ni)], load_sem.at[0])]
            + [pltpu.make_async_copy(lin1.at[q, aligned(peer1[n], ni), :, lanes], vin1.at[aligned(peer1[n], ni)], load_sem.at[n + 1])
               for n in range(n1 - 1)])
        full = n1 * ni
        part = 32

        @pl.loop(0, full // part)
        def _(b):
            vscr[aligned(b, part * jc), :] = vin1[pl.ds(b * part, part)].astype(F32).reshape(part * jc, LANES)

        @pl.loop(0, jc // 2)
        def _(b):
            rows = [pl.ds(2 * b + e, full, stride=jc) for e in range(2)]
            rhs_mat = jnp.concatenate([vscr[row, :].astype(BF16) for row in rows], axis=1)
            res = jnp.dot(mat[...], rhs_mat, preferred_element_type=F32)
            for e in range(2):
                vscr[rows[e], :] = res[:, e * LANES:(e + 1) * LANES]

        @pl.loop(0, full // part)
        def _(b):
            vout1[pl.ds(b * part, part)] = vscr[aligned(b, part * jc), :].reshape(part, jc, LANES).astype(BF16)

        stores = [pltpu.make_async_copy(vout1.at[aligned(peer1[n], ni)], out1.at[g, aligned(peer1[n], ni)], store_sem.at[n + 1])
                  for n in range(n1 - 1)]
        if not is_last(stage, c):
            stores += [pltpu.make_async_copy(vout1.at[aligned(me1, ni)], t1.at[g, :, aligned(me1, jc), :], store_sem.at[0])]
        run(stores)
        for n in order1:
            back_y(stage, c, n).start()

    def product_two(stage, r, h, c):
        q, g, lanes = stage * rhs + r, stage * chunks + c, aligned(h, LANES)
        mat = (ma2, mb2)[stage]
        run([pltpu.make_async_copy(field(stage, r).at[aligned(me2, ic), :, lanes], vin2.at[:, aligned(me2, nj), :], load_sem.at[0])]
            + [pltpu.make_async_copy(lin2.at[q, :, aligned(peer2[n], nj), lanes], vin2.at[:, aligned(peer2[n], nj), :], load_sem.at[n + 1])
               for n in range(n2 - 1)])

        @pl.loop(0, ic // 2)
        def _(b):
            rhs_mat = jnp.concatenate([vin2[2 * b], vin2[2 * b + 1]], axis=1)
            res = jnp.dot(mat[...], rhs_mat, preferred_element_type=F32).astype(BF16)
            vout2[2 * b] = res[:, :LANES]
            vout2[2 * b + 1] = res[:, LANES:]

        stores = [pltpu.make_async_copy(vout2.at[:, aligned(peer2[n], nj), :], out2.at[g, :, aligned(peer2[n], nj), :], store_sem.at[n + 1])
                  for n in range(n2 - 1)]
        if not is_last(stage, c):
            stores += [pltpu.make_async_copy(vout2.at[:, aligned(me2, nj), :], t2.at[g, aligned(me2, ic)], store_sem.at[0])]
        run(stores)
        for n in order2:
            back_x(stage, c, n).start()

    def products(stage, r, h):
        c = r * halves + h
        product_one(stage, r, h, c)
        product_two(stage, r, h, c)

    def third(stage, h, put):
        mat = (ma3, mb3)[stage]
        rows = pl.ds(pl.multiple_of(me3 * nk + h * LANES, LANES), LANES)
        mat_own = mat[rows, aligned(me3, nk)]
        mat_par = mat[rows, aligned(peer3, nk)]
        contract = (((1,), (1,)), ((), ()))
        part = 8

        @pl.loop(0, ni // part)
        def _(b):
            sel = pl.ds(b * part, part)
            term = lax.dot_general(vown[sel].reshape(part * nj, nk), mat_own, contract, preferred_element_type=F32)
            term += lax.dot_general(vpar[sel].reshape(part * nj, nk), mat_par, contract, preferred_element_type=F32)
            put(sel, term.astype(BF16).astype(F32).reshape(part, nj, LANES))

    def load_field(stage, r):
        return [pltpu.make_async_copy(field(stage, r), vown, load_sem.at[2]),
                pltpu.make_async_copy(lin3.at[stage * rhs + r], vpar, load_sem.at[3])]

    def load_terms(stage, c):
        g = stage * chunks + c
        return [pltpu.make_async_copy(t1.at[g], v1, load_sem.at[0]), pltpu.make_async_copy(t2.at[g], v2, load_sem.at[1])]

    def total_a(r, h):
        c, lanes = r * halves + h, aligned(h, LANES)
        wait_back(0, c)
        run(load_terms(0, c) + load_field(0, r) + [pltpu.make_async_copy(d_ref.at[:, :, lanes], vd, load_sem.at[4])])

        def put(sel, term):
            acc = v1[sel].astype(F32) + v2[sel].astype(F32) + term
            vw[sel] = (vd[sel] * acc.astype(BF16).astype(F32)).astype(BF16)

        third(0, h, put)
        run([pltpu.make_async_copy(vw, w.at[r, :, :, lanes], store_sem.at[0])])

    def third_b(r, h):
        run(load_field(1, r))

        def put(sel, term):
            z_ref[r, sel, :, aligned(h, LANES)] = term

        third(1, h, put)

    def total_b(r, h):
        c = r * halves + h
        third_b(r, h)
        wait_back(1, c)
        run(load_terms(1, c))
        part = 8

        @pl.loop(0, ni // part)
        def _(b):
            sel = pl.ds(b * part, part)
            z_ref[r, sel, :, aligned(h, LANES)] = (v1[sel].astype(F32) + v2[sel].astype(F32)) + z_ref[r, sel, :, aligned(h, LANES)]

    def total_last(r, h):
        c, lanes = r * halves + h, pl.ds(h * LANES, LANES)
        third_b(r, h)
        part = 16

        @pl.loop(0, ni // part)
        def _(b):
            last1[pl.ds(b * part, part), aligned(me1, jc), :] = vout1[pl.ds(me1 * ni + b * part, part)]

        @pl.loop(0, ic // part)
        def _(b):
            last2[pl.ds(me2 * ic + b * part, part)] = vout2[pl.ds(b * part, part), aligned(me2, nj), :]

        def tile(i_block, cols, part):
            @pl.loop(0, ic // part)
            def _(b):
                sel = pl.ds(i_block * ic + b * part, part)
                z_ref[r, sel, cols, lanes] = (last1[sel, cols, :].astype(F32) + last2[sel, cols, :].astype(F32)) + z_ref[r, sel, cols, lanes]

        @pl.loop(0, rhs)
        def _(e):
            wait_out_sends(0, e)
            wait_out_sends(1, e)

        @pl.loop(0, chunks)
        def _(e):
            wait_back_sends(0, e)

        @pl.loop(0, chunks - 1)
        def _(e):
            wait_back_sends(1, e)

        j_blocks = [me1] + [peer1[n1 - 2 - n] for n in order1]
        i_blocks = [me2] + [peer2[n2 - 2 - n] for n in order2]
        for m in range(max(n1, n2)):
            if m < n1:
                if m > 0:
                    back_y(1, c, order1[m - 1]).wait_recv()
                for e in range(min(m, n2)):
                    tile(i_blocks[e], aligned(j_blocks[m], jc), part)
            if m < n2:
                if m > 0:
                    back_x(1, c, order2[m - 1]).wait_recv()
                if m + 1 >= n1:
                    tile(i_blocks[m], slice(None), part // 2)
                else:
                    for e in range(m + 1):
                        tile(i_blocks[m], aligned(j_blocks[e], jc), part)
        wait_back_sends(1, c)

    @pl.loop(0, rhs)
    def _(r):
        start_out(0, r)

    run([pltpu.make_async_copy(src, dst, mat_sem.at[m]) for m, (src, dst) in enumerate(
        zip((a1_ref, a2_ref, a3_ref, b1_ref, b2_ref, b3_ref), (ma1, ma2, ma3, mb1, mb2, mb3)))])

    @pl.loop(0, rhs)
    def _(r):
        wait_out(0, r)

        @pl.loop(0, halves)
        def _(h):
            products(0, r, h)

    @pl.loop(0, rhs)
    def _(r):
        out_c(0, r).wait_recv()

        @pl.loop(0, halves)
        def _(h):
            total_a(r, h)

        start_out(1, r)

    @pl.loop(0, rhs - 1)
    def _(r):
        wait_out(1, r)

        @pl.loop(0, halves)
        def _(h):
            products(1, r, h)

    wait_out(1, rhs - 1)

    @pl.loop(0, halves - 1)
    def _(h):
        products(1, rhs - 1, h)

    products(1, rhs - 1, halves - 1)

    @pl.loop(0, rhs)
    def _(r):
        out_c(1, r).wait_recv()

    @pl.loop(0, chunks - 1)
    def _(c):
        total_b(c // halves, lax.rem(c, halves))

    total_last(rhs - 1, halves - 1)


def write_out(z_in, z_out, sem):
    rhs, parts = sem.shape
    size = z_in.shape[1] // parts
    copies = [pltpu.make_async_copy(z_in.at[r, pl.ds(b * size, size)], z_out.at[r, pl.ds(b * size, size)], sem.at[r, b])
              for r in range(rhs) for b in range(parts)]
    for copy in copies:
        copy.start()
    for copy in copies:
        copy.wait()


def solution(mesh):
    n1, n2, n3 = mesh.shape['mode1'], mesh.shape['mode2'], mesh.shape['mode3']
    vol_spec = P('rhs', 'mode1', 'mode2', 'mode3')
    diag_spec = P('mode1', 'mode2', 'mode3')

    def local_op(x_vol, diag_vals, *mats):
        rhs, ni, nj, nk = x_vol.shape
        dims = (n1, n2, n3, rhs, ni, nj, nk)
        halves = nk // LANES
        chunks = rhs * halves
        jc, ic = nj // n1, ni // n2
        hbm = pl.BlockSpec(memory_space=pltpu.HBM)
        vmem = pl.BlockSpec(memory_space=pltpu.VMEM)
        dma = pltpu.SemaphoreType.DMA
        block = (ni, nj, LANES)
        outs = [
            pltpu.VMEM(x_vol.shape, F32),
            jax.ShapeDtypeStruct((2 * rhs, n1 * ni, jc, nk), BF16),
            jax.ShapeDtypeStruct((2 * rhs, ic, n2 * nj, nk), BF16),
            jax.ShapeDtypeStruct((2 * rhs, ni, nj, nk), BF16),
            jax.ShapeDtypeStruct((2 * chunks, n1 * ni, jc, LANES), BF16),
            jax.ShapeDtypeStruct((2 * chunks, ic, n2 * nj, LANES), BF16),
            jax.ShapeDtypeStruct((2 * chunks,) + block, BF16),
            jax.ShapeDtypeStruct((2 * chunks,) + block, BF16),
            jax.ShapeDtypeStruct(x_vol.shape, BF16),
        ]
        scratch = [pltpu.VMEM(mat.shape, mat.dtype) for mat in mats] + [
            pltpu.VMEM((n1 * ni, jc, LANES), BF16),
            pltpu.VMEM((n1 * ni * jc, LANES), F32),
            pltpu.VMEM((n1 * ni, jc, LANES), BF16),
            pltpu.VMEM((ic, n2 * nj, LANES), BF16),
            pltpu.VMEM((ic, n2 * nj, LANES), BF16),
            pltpu.VMEM(block, BF16),
            pltpu.VMEM(block, BF16),
            pltpu.VMEM((ni, nj, nk), BF16),
            pltpu.VMEM((ni, nj, nk), BF16),
            pltpu.VMEM(block, F32),
            pltpu.VMEM(block, BF16),
            pltpu.VMEM(block, BF16),
            pltpu.VMEM(block, BF16),
            dma((2 * rhs, n1 - 1)), dma((2 * rhs, n1 - 1)),
            dma((2 * rhs, n2 - 1)), dma((2 * rhs, n2 - 1)),
            dma((2 * rhs,)), dma((2 * rhs,)),
            dma((2 * chunks, n1 - 1)), dma((2 * chunks, n1 - 1)),
            dma((2 * chunks, n2 - 1)), dma((2 * chunks, n2 - 1)),
            dma((len(mats),)), dma((max(5, n1, n2),)), dma((max(n1, n2),)),
        ]
        z_vol = pl.pallas_call(
            functools.partial(kernel, dims),
            out_shape=outs,
            in_specs=[hbm] * (2 + len(mats)),
            out_specs=[vmem] + [hbm] * (len(outs) - 1),
            scratch_shapes=scratch,
            compiler_params=pltpu.CompilerParams(collective_id=0, has_side_effects=True, vmem_limit_bytes=46 * 2 ** 20),
        )(x_vol, diag_vals, *mats)[0]
        return pl.pallas_call(
            write_out,
            out_shape=jax.ShapeDtypeStruct(x_vol.shape, F32),
            in_specs=[vmem],
            out_specs=hbm,
            scratch_shapes=[dma((rhs, 8))],
            compiler_params=pltpu.CompilerParams(vmem_limit_bytes=24 * 2 ** 20),
        )(z_vol)

    return jax.shard_map(local_op, mesh=mesh, in_specs=(vol_spec, diag_spec, P(), P(), P(), P(), P(), P()), out_specs=vol_spec, check_vma=False)
```

```python
import functools

import jax
import jax.numpy as jnp
from jax import lax
from jax.experimental import pallas as pl
from jax.experimental.pallas import tpu as pltpu
from jax.sharding import PartitionSpec as P

MESH = pl.DeviceIdType.MESH
F32, BF16 = jnp.float32, jnp.bfloat16
LANES = 128


def aligned(index, size):
    return pl.ds(pl.multiple_of(index * size, size), size)


def kernel(dims, x_ref, d_ref, a1_ref, a2_ref, a3_ref, b1_ref, b2_ref, b3_ref,
           z_ref, lin1, lin2, lin3, out1, out2, t1, t2, w,
           ma1, ma2, ma3, mb1, mb2, mb3,
           vin1, vscr, vout1, vin2, vout2, v1, v2, vown, vpar, vd, vw, last1, last2,
           y_send, y_recv, x_send, x_recv, c_send, c_recv,
           y_send2, y_recv2, x_send2, x_recv2, mat_sem, load_sem, store_sem):
    n1, n2, n3, rhs, ni, nj, nk = dims
    halves = nk // LANES
    jc, ic = nj // n1, ni // n2
    me1, me2, me3 = lax.axis_index('mode1'), lax.axis_index('mode2'), lax.axis_index('mode3')
    peer1 = [lax.rem(me1 + s, n1) for s in range(1, n1)]
    peer2 = [lax.rem(me2 + s, n2) for s in range(1, n2)]
    peer3 = lax.rem(me3 + 1, n3)

    barrier = pltpu.get_barrier_semaphore()
    for axis, peers in (('mode1', peer1), ('mode2', peer2), ('mode3', [peer3])):
        for peer in peers:
            pl.semaphore_signal(barrier, inc=1, device_id={axis: peer}, device_id_type=MESH)
    pl.semaphore_wait(barrier, n1 + n2 + n3 - 3)

    order1 = sorted(range(n1 - 1), key=lambda n: min(n + 1, n1 - n - 1))
    order2 = sorted(range(n2 - 1), key=lambda n: min(n + 1, n2 - n - 1))

    def remote(src, dst, send, recv, axis, peer):
        return pltpu.make_async_remote_copy(src_ref=src, dst_ref=dst, send_sem=send, recv_sem=recv,
                                            device_id={axis: peer}, device_id_type=MESH)

    def run(copies):
        for copy in copies:
            copy.start()
        for copy in copies:
            copy.wait()

    def field(stage, r):
        return (x_ref, w)[stage].at[r]

    def out_y(stage, r, n):
        q = stage * rhs + r
        return remote(field(stage, r).at[:, aligned(peer1[n], jc), :], lin1.at[q, aligned(me1, ni)],
                      y_send.at[q, n], y_recv.at[q, n], 'mode1', peer1[n])

    def out_x(stage, r, n):
        q = stage * rhs + r
        return remote(field(stage, r).at[aligned(peer2[n], ic)], lin2.at[q, :, aligned(me2, nj), :],
                      x_send.at[q, n], x_recv.at[q, n], 'mode2', peer2[n])

    def out_c(stage, r):
        q = stage * rhs + r
        return remote(field(stage, r), lin3.at[q], c_send.at[q], c_recv.at[q], 'mode3', peer3)

    def back_y(stage, r, n, h=None):
        q = stage * rhs + r
        row, lanes = (q, slice(None)) if h is None else (2 * rhs - 1 + h, aligned(h, LANES))
        dst = last1 if is_last(h) else t1.at[q, :, :, lanes]
        return remote(out1.at[q, aligned(peer1[n], ni), :, lanes], dst.at[:, aligned(me1, jc), :],
                      y_send2.at[row, n], y_recv2.at[row, n], 'mode1', peer1[n])

    def back_x(stage, r, n, h=None):
        q = stage * rhs + r
        row, lanes = (q, slice(None)) if h is None else (2 * rhs - 1 + h, aligned(h, LANES))
        dst = last2 if is_last(h) else t2.at[q, :, :, lanes]
        return remote(out2.at[q, :, aligned(peer2[n], nj), lanes], dst.at[aligned(me2, ic)],
                      x_send2.at[row, n], x_recv2.at[row, n], 'mode2', peer2[n])

    def is_last(h):
        return isinstance(h, int) and h == halves - 1

    def start_back(stage, r, h=None):
        for n in order1:
            back_y(stage, r, n, h).start()
        for n in order2:
            back_x(stage, r, n, h).start()

    def start_out(stage, r):
        for n in order1:
            out_y(stage, r, n).start()
        for n in order2:
            out_x(stage, r, n).start()
        out_c(stage, r).start()

    def wait_out(stage, r):
        for n in range(n1 - 1):
            out_y(stage, r, n).wait_recv()
        for n in range(n2 - 1):
            out_x(stage, r, n).wait_recv()

    def wait_back(stage, r, h=None):
        for n in range(n1 - 1):
            back_y(stage, r, n, h).wait_recv()
        for n in range(n2 - 1):
            back_x(stage, r, n, h).wait_recv()

    def wait_out_sends(stage, r):
        for n in range(n1 - 1):
            out_y(stage, r, n).wait_send()
        for n in range(n2 - 1):
            out_x(stage, r, n).wait_send()
        out_c(stage, r).wait_send()

    def wait_back_sends(stage, r, h=None):
        for n in range(n1 - 1):
            back_y(stage, r, n, h).wait_send()
        for n in range(n2 - 1):
            back_x(stage, r, n, h).wait_send()

    def product_one(stage, r, h, last):
        q, lanes = stage * rhs + r, aligned(h, LANES)
        mat = (ma1, mb1)[stage]
        run([pltpu.make_async_copy(field(stage, r).at[:, aligned(me1, jc), lanes], vin1.at[aligned(me1, ni)], load_sem.at[0])]
            + [pltpu.make_async_copy(lin1.at[q, aligned(peer1[n], ni), :, lanes], vin1.at[aligned(peer1[n], ni)], load_sem.at[n + 1])
               for n in range(n1 - 1)])
        full = n1 * ni
        part = 32

        @pl.loop(0, full // part)
        def _(b):
            vscr[aligned(b, part * jc), :] = vin1[pl.ds(b * part, part)].astype(F32).reshape(part * jc, LANES)

        @pl.loop(0, jc // 2)
        def _(b):
            rows = [pl.ds(2 * b + e, full, stride=jc) for e in range(2)]
            rhs_mat = jnp.concatenate([vscr[row, :].astype(BF16) for row in rows], axis=1)
            res = jnp.dot(mat[...], rhs_mat, preferred_element_type=F32)
            for e in range(2):
                vscr[rows[e], :] = res[:, e * LANES:(e + 1) * LANES]

        @pl.loop(0, full // part)
        def _(b):
            vout1[pl.ds(b * part, part)] = vscr[aligned(b, part * jc), :].reshape(part, jc, LANES).astype(BF16)

        stores = [pltpu.make_async_copy(vout1.at[aligned(peer1[n], ni)], out1.at[q, aligned(peer1[n], ni), :, lanes], store_sem.at[n + 1])
                  for n in range(n1 - 1)]
        if not last:
            stores += [pltpu.make_async_copy(vout1.at[aligned(me1, ni)], t1.at[q, :, aligned(me1, jc), lanes], store_sem.at[0])]
        run(stores)

    def product_two(stage, r, h, last):
        q, lanes = stage * rhs + r, aligned(h, LANES)
        mat = (ma2, mb2)[stage]
        run([pltpu.make_async_copy(field(stage, r).at[aligned(me2, ic), :, lanes], vin2.at[:, aligned(me2, nj), :], load_sem.at[0])]
            + [pltpu.make_async_copy(lin2.at[q, :, aligned(peer2[n], nj), lanes], vin2.at[:, aligned(peer2[n], nj), :], load_sem.at[n + 1])
               for n in range(n2 - 1)])

        @pl.loop(0, ic // 2)
        def _(b):
            rhs_mat = jnp.concatenate([vin2[2 * b], vin2[2 * b + 1]], axis=1)
            res = jnp.dot(mat[...], rhs_mat, preferred_element_type=F32).astype(BF16)
            vout2[2 * b] = res[:, :LANES]
            vout2[2 * b + 1] = res[:, LANES:]

        stores = [pltpu.make_async_copy(vout2.at[:, aligned(peer2[n], nj), :], out2.at[q, :, aligned(peer2[n], nj), lanes], store_sem.at[n + 1])
                  for n in range(n2 - 1)]
        if not last:
            stores += [pltpu.make_async_copy(vout2.at[:, aligned(me2, nj), :], t2.at[q, aligned(me2, ic), :, lanes], store_sem.at[0])]
        run(stores)

    def products(stage, r, h, last=False):
        product_one(stage, r, h, last)
        product_two(stage, r, h, last)

    def third(stage, h, put):
        mat = (ma3, mb3)[stage]
        rows = pl.ds(pl.multiple_of(me3 * nk + h * LANES, LANES), LANES)
        mat_own = mat[rows, aligned(me3, nk)]
        mat_par = mat[rows, aligned(peer3, nk)]
        contract = (((1,), (1,)), ((), ()))
        part = 8

        @pl.loop(0, ni // part)
        def _(b):
            sel = pl.ds(b * part, part)
            term = lax.dot_general(vown[sel].reshape(part * nj, nk), mat_own, contract, preferred_element_type=F32)
            term += lax.dot_general(vpar[sel].reshape(part * nj, nk), mat_par, contract, preferred_element_type=F32)
            put(sel, term.astype(BF16).astype(F32).reshape(part, nj, LANES))

    def load_field(stage, r):
        return [pltpu.make_async_copy(field(stage, r), vown, load_sem.at[2]),
                pltpu.make_async_copy(lin3.at[stage * rhs + r], vpar, load_sem.at[3])]

    def load_terms(stage, r, h):
        q, lanes = stage * rhs + r, aligned(h, LANES)
        return [pltpu.make_async_copy(t1.at[q, :, :, lanes], v1, load_sem.at[0]), pltpu.make_async_copy(t2.at[q, :, :, lanes], v2, load_sem.at[1])]

    def total_a(r, h):
        lanes = aligned(h, LANES)
        run(load_terms(0, r, h) + load_field(0, r) + [pltpu.make_async_copy(d_ref.at[:, :, lanes], vd, load_sem.at[4])])

        def put(sel, term):
            acc = v1[sel].astype(F32) + v2[sel].astype(F32) + term
            vw[sel] = (vd[sel] * acc.astype(BF16).astype(F32)).astype(BF16)

        third(0, h, put)
        run([pltpu.make_async_copy(vw, w.at[r, :, :, lanes], store_sem.at[0])])

    def third_b(r, h):
        run(load_field(1, r))

        def put(sel, term):
            z_ref[r, sel, :, aligned(h, LANES)] = term

        third(1, h, put)

    def total_b(r, h):
        run(load_terms(1, r, h))
        part = 8

        @pl.loop(0, ni // part)
        def _(b):
            sel = pl.ds(b * part, part)
            z_ref[r, sel, :, aligned(h, LANES)] = (v1[sel].astype(F32) + v2[sel].astype(F32)) + z_ref[r, sel, :, aligned(h, LANES)]

    def total_last(r, h):
        lanes = pl.ds(h * LANES, LANES)
        third_b(r, h)
        part = 16

        @pl.loop(0, ni // part)
        def _(b):
            last1[pl.ds(b * part, part), aligned(me1, jc), :] = vout1[pl.ds(me1 * ni + b * part, part)]

        @pl.loop(0, ic // part)
        def _(b):
            last2[pl.ds(me2 * ic + b * part, part)] = vout2[pl.ds(b * part, part), aligned(me2, nj), :]

        def tile(i_block, cols, part):
            @pl.loop(0, ic // part)
            def _(b):
                sel = pl.ds(i_block * ic + b * part, part)
                z_ref[r, sel, cols, lanes] = (last1[sel, cols, :].astype(F32) + last2[sel, cols, :].astype(F32)) + z_ref[r, sel, cols, lanes]

        @pl.loop(0, rhs)
        def _(e):
            wait_out_sends(0, e)
            wait_out_sends(1, e)
            wait_back_sends(0, e)

        @pl.loop(0, rhs - 1)
        def _(e):
            wait_back_sends(1, e)

        @pl.loop(0, halves - 1)
        def _(e):
            wait_back_sends(1, r, e)

        j_blocks = [me1] + [peer1[n1 - 2 - n] for n in order1]
        i_blocks = [me2] + [peer2[n2 - 2 - n] for n in order2]
        for m in range(max(n1, n2)):
            if m < n1:
                if m > 0:
                    back_y(1, r, order1[m - 1], h).wait_recv()
                for e in range(min(m, n2)):
                    tile(i_blocks[e], aligned(j_blocks[m], jc), part)
            if m < n2:
                if m > 0:
                    back_x(1, r, order2[m - 1], h).wait_recv()
                if m + 1 >= n1:
                    tile(i_blocks[m], slice(None), part // 2)
                else:
                    for e in range(m + 1):
                        tile(i_blocks[m], aligned(j_blocks[e], jc), part)
        wait_back_sends(1, r, h)

    @pl.loop(0, rhs)
    def _(r):
        start_out(0, r)

    run([pltpu.make_async_copy(src, dst, mat_sem.at[m]) for m, (src, dst) in enumerate(
        zip((a1_ref, a2_ref, a3_ref, b1_ref, b2_ref, b3_ref), (ma1, ma2, ma3, mb1, mb2, mb3)))])

    @pl.loop(0, rhs)
    def _(r):
        wait_out(0, r)

        @pl.loop(0, halves)
        def _(h):
            products(0, r, h)

        start_back(0, r)

    @pl.loop(0, rhs)
    def _(r):
        out_c(0, r).wait_recv()
        wait_back(0, r)

        @pl.loop(0, halves)
        def _(h):
            total_a(r, h)

        start_out(1, r)

    @pl.loop(0, rhs - 1)
    def _(r):
        wait_out(1, r)

        @pl.loop(0, halves)
        def _(h):
            products(1, r, h)

        start_back(1, r)

    end = rhs - 1
    wait_out(1, end)

    @pl.loop(0, halves - 1)
    def _(h):
        products(1, end, h)
        start_back(1, end, h)

    products(1, end, halves - 1, True)
    start_back(1, end, halves - 1)

    @pl.loop(0, rhs)
    def _(r):
        out_c(1, r).wait_recv()

    @pl.loop(0, rhs - 1)
    def _(r):
        @pl.loop(0, halves)
        def _(h):
            third_b(r, h)

        wait_back(1, r)

        @pl.loop(0, halves)
        def _(h):
            total_b(r, h)

    @pl.loop(0, halves - 1)
    def _(h):
        third_b(end, h)
        wait_back(1, end, h)
        total_b(end, h)

    total_last(end, halves - 1)


def write_out(z_in, z_out, sem):
    rhs, parts = sem.shape
    size = z_in.shape[1] // parts
    copies = [pltpu.make_async_copy(z_in.at[r, pl.ds(b * size, size)], z_out.at[r, pl.ds(b * size, size)], sem.at[r, b])
              for r in range(rhs) for b in range(parts)]
    for copy in copies:
        copy.start()
    for copy in copies:
        copy.wait()


def solution(mesh):
    n1, n2, n3 = mesh.shape['mode1'], mesh.shape['mode2'], mesh.shape['mode3']
    vol_spec = P('rhs', 'mode1', 'mode2', 'mode3')
    diag_spec = P('mode1', 'mode2', 'mode3')

    def local_op(x_vol, diag_vals, *mats):
        rhs, ni, nj, nk = x_vol.shape
        dims = (n1, n2, n3, rhs, ni, nj, nk)
        halves = nk // LANES
        backs = 2 * rhs - 1 + halves
        jc, ic = nj // n1, ni // n2
        hbm = pl.BlockSpec(memory_space=pltpu.HBM)
        vmem = pl.BlockSpec(memory_space=pltpu.VMEM)
        dma = pltpu.SemaphoreType.DMA
        block = (ni, nj, LANES)
        outs = [
            pltpu.VMEM(x_vol.shape, F32),
            jax.ShapeDtypeStruct((2 * rhs, n1 * ni, jc, nk), BF16),
            jax.ShapeDtypeStruct((2 * rhs, ic, n2 * nj, nk), BF16),
            jax.ShapeDtypeStruct((2 * rhs, ni, nj, nk), BF16),
            jax.ShapeDtypeStruct((2 * rhs, n1 * ni, jc, nk), BF16),
            jax.ShapeDtypeStruct((2 * rhs, ic, n2 * nj, nk), BF16),
            jax.ShapeDtypeStruct((2 * rhs, ni, nj, nk), BF16),
            jax.ShapeDtypeStruct((2 * rhs, ni, nj, nk), BF16),
            jax.ShapeDtypeStruct(x_vol.shape, BF16),
        ]
        scratch = [pltpu.VMEM(mat.shape, mat.dtype) for mat in mats] + [
            pltpu.VMEM((n1 * ni, jc, LANES), BF16),
            pltpu.VMEM((n1 * ni * jc, LANES), F32),
            pltpu.VMEM((n1 * ni, jc, LANES), BF16),
            pltpu.VMEM((ic, n2 * nj, LANES), BF16),
            pltpu.VMEM((ic, n2 * nj, LANES), BF16),
            pltpu.VMEM(block, BF16),
            pltpu.VMEM(block, BF16),
            pltpu.VMEM((ni, nj, nk), BF16),
            pltpu.VMEM((ni, nj, nk), BF16),
            pltpu.VMEM(block, F32),
            pltpu.VMEM(block, BF16),
            pltpu.VMEM(block, BF16),
            pltpu.VMEM(block, BF16),
            dma((2 * rhs, n1 - 1)), dma((2 * rhs, n1 - 1)),
            dma((2 * rhs, n2 - 1)), dma((2 * rhs, n2 - 1)),
            dma((2 * rhs,)), dma((2 * rhs,)),
            dma((backs, n1 - 1)), dma((backs, n1 - 1)),
            dma((backs, n2 - 1)), dma((backs, n2 - 1)),
            dma((len(mats),)), dma((max(5, n1, n2),)), dma((max(n1, n2),)),
        ]
        z_vol = pl.pallas_call(
            functools.partial(kernel, dims),
            out_shape=outs,
            in_specs=[hbm] * (2 + len(mats)),
            out_specs=[vmem] + [hbm] * (len(outs) - 1),
            scratch_shapes=scratch,
            compiler_params=pltpu.CompilerParams(collective_id=0, has_side_effects=True, vmem_limit_bytes=46 * 2 ** 20),
        )(x_vol, diag_vals, *mats)[0]
        return pl.pallas_call(
            write_out,
            out_shape=jax.ShapeDtypeStruct(x_vol.shape, F32),
            in_specs=[vmem],
            out_specs=hbm,
            scratch_shapes=[dma((rhs, 4))],
            compiler_params=pltpu.CompilerParams(vmem_limit_bytes=24 * 2 ** 20),
        )(z_vol)

    return jax.shard_map(local_op, mesh=mesh, in_specs=(vol_spec, diag_spec, P(), P(), P(), P(), P(), P()), out_specs=vol_spec, check_vma=False)
```

```python
import functools

import jax
import jax.numpy as jnp
from jax import lax
from jax.experimental import pallas as pl
from jax.experimental.pallas import tpu as pltpu
from jax.sharding import PartitionSpec as P

MESH = pl.DeviceIdType.MESH
F32, BF16 = jnp.float32, jnp.bfloat16
LANES = 128


def aligned(index, size):
    return pl.ds(pl.multiple_of(index * size, size), size)


def kernel(dims, x_ref, d_ref, a1_ref, a2_ref, a3_ref, b1_ref, b2_ref, b3_ref,
           z_ref, lin1, lin2, lin3, out1, out2, t1, t2, w,
           ma1, ma2, ma3, mb1, mb2, mb3,
           vin1, vscr, vout1, vin2, vout2, v1, v2, vown, vpar, vd, vw, last1, last2,
           y_send, y_recv, x_send, x_recv, c_send, c_recv,
           y_send2, y_recv2, x_send2, x_recv2, mat_sem, load_sem, store_sem):
    n1, n2, n3, rhs, ni, nj, nk = dims
    halves = nk // LANES
    jc, ic = nj // n1, ni // n2
    me1, me2, me3 = lax.axis_index('mode1'), lax.axis_index('mode2'), lax.axis_index('mode3')
    peer1 = [lax.rem(me1 + s, n1) for s in range(1, n1)]
    peer2 = [lax.rem(me2 + s, n2) for s in range(1, n2)]
    peer3 = lax.rem(me3 + 1, n3)

    barrier = pltpu.get_barrier_semaphore()
    for axis, peers in (('mode1', peer1), ('mode2', peer2), ('mode3', [peer3])):
        for peer in peers:
            pl.semaphore_signal(barrier, inc=1, device_id={axis: peer}, device_id_type=MESH)
    pl.semaphore_wait(barrier, n1 + n2 + n3 - 3)

    order1 = sorted(range(n1 - 1), key=lambda n: min(n + 1, n1 - n - 1))
    order2 = sorted(range(n2 - 1), key=lambda n: min(n + 1, n2 - n - 1))

    def remote(src, dst, send, recv, axis, peer):
        return pltpu.make_async_remote_copy(src_ref=src, dst_ref=dst, send_sem=send, recv_sem=recv,
                                            device_id={axis: peer}, device_id_type=MESH)

    def run(copies):
        for copy in copies:
            copy.start()
        for copy in copies:
            copy.wait()

    def field(stage, r):
        return (x_ref, w)[stage].at[r]

    def out_y(stage, r, n):
        q = stage * rhs + r
        return remote(field(stage, r).at[:, aligned(peer1[n], jc), :], lin1.at[q, aligned(me1, ni)],
                      y_send.at[q, n], y_recv.at[q, n], 'mode1', peer1[n])

    def out_x(stage, r, n):
        q = stage * rhs + r
        return remote(field(stage, r).at[aligned(peer2[n], ic)], lin2.at[q, :, aligned(me2, nj), :],
                      x_send.at[q, n], x_recv.at[q, n], 'mode2', peer2[n])

    def out_c(stage, r):
        q = stage * rhs + r
        return remote(field(stage, r), lin3.at[q], c_send.at[q], c_recv.at[q], 'mode3', peer3)

    def back_y(stage, r, n, h=None):
        q = stage * rhs + r
        row, lanes = (q, slice(None)) if h is None else (2 * rhs - 1 + h, aligned(h, LANES))
        dst = last1 if is_last(h) else t1.at[q, :, :, lanes]
        return remote(out1.at[q, aligned(peer1[n], ni), :, lanes], dst.at[:, aligned(me1, jc), :],
                      y_send2.at[row, n], y_recv2.at[row, n], 'mode1', peer1[n])

    def back_x(stage, r, n, h=None):
        q = stage * rhs + r
        row, lanes = (q, slice(None)) if h is None else (2 * rhs - 1 + h, aligned(h, LANES))
        dst = last2 if is_last(h) else t2.at[q, :, :, lanes]
        return remote(out2.at[q, :, aligned(peer2[n], nj), lanes], dst.at[aligned(me2, ic)],
                      x_send2.at[row, n], x_recv2.at[row, n], 'mode2', peer2[n])

    def is_last(h):
        return isinstance(h, int) and h == halves - 1

    def start_back_y(stage, r, h=None):
        for n in order1:
            back_y(stage, r, n, h).start()

    def start_back_x(stage, r, h=None):
        for n in order2:
            back_x(stage, r, n, h).start()

    def start_out(stage, r):
        for n in order1:
            out_y(stage, r, n).start()
        for n in order2:
            out_x(stage, r, n).start()
        out_c(stage, r).start()

    def wait_out_y(stage, r):
        for n in range(n1 - 1):
            out_y(stage, r, n).wait_recv()

    def wait_out_x(stage, r):
        for n in range(n2 - 1):
            out_x(stage, r, n).wait_recv()

    def wait_back(stage, r, h=None):
        for n in range(n1 - 1):
            back_y(stage, r, n, h).wait_recv()
        for n in range(n2 - 1):
            back_x(stage, r, n, h).wait_recv()

    def wait_out_sends(stage, r):
        for n in range(n1 - 1):
            out_y(stage, r, n).wait_send()
        for n in range(n2 - 1):
            out_x(stage, r, n).wait_send()
        out_c(stage, r).wait_send()

    def wait_back_sends(stage, r, h=None):
        for n in range(n1 - 1):
            back_y(stage, r, n, h).wait_send()
        for n in range(n2 - 1):
            back_x(stage, r, n, h).wait_send()

    def product_one(stage, r, h, last):
        q, lanes = stage * rhs + r, aligned(h, LANES)
        mat = (ma1, mb1)[stage]
        run([pltpu.make_async_copy(field(stage, r).at[:, aligned(me1, jc), lanes], vin1.at[aligned(me1, ni)], load_sem.at[0])]
            + [pltpu.make_async_copy(lin1.at[q, aligned(peer1[n], ni), :, lanes], vin1.at[aligned(peer1[n], ni)], load_sem.at[n + 1])
               for n in range(n1 - 1)])
        full = n1 * ni
        part = 32

        @pl.loop(0, full // part)
        def _(b):
            vscr[aligned(b, part * jc), :] = vin1[pl.ds(b * part, part)].astype(F32).reshape(part * jc, LANES)

        @pl.loop(0, jc // 2)
        def _(b):
            rows = [pl.ds(2 * b + e, full, stride=jc) for e in range(2)]
            rhs_mat = jnp.concatenate([vscr[row, :].astype(BF16) for row in rows], axis=1)
            res = jnp.dot(mat[...], rhs_mat, preferred_element_type=F32)
            for e in range(2):
                vscr[rows[e], :] = res[:, e * LANES:(e + 1) * LANES]

        @pl.loop(0, full // part)
        def _(b):
            vout1[pl.ds(b * part, part)] = vscr[aligned(b, part * jc), :].reshape(part, jc, LANES).astype(BF16)

        stores = [pltpu.make_async_copy(vout1.at[aligned(peer1[n], ni)], out1.at[q, aligned(peer1[n], ni), :, lanes], store_sem.at[n + 1])
                  for n in range(n1 - 1)]
        if not last:
            stores += [pltpu.make_async_copy(vout1.at[aligned(me1, ni)], t1.at[q, :, aligned(me1, jc), lanes], store_sem.at[0])]
        run(stores)

    def product_two(stage, r, h, last):
        q, lanes = stage * rhs + r, aligned(h, LANES)
        mat = (ma2, mb2)[stage]
        run([pltpu.make_async_copy(field(stage, r).at[aligned(me2, ic), :, lanes], vin2.at[:, aligned(me2, nj), :], load_sem.at[0])]
            + [pltpu.make_async_copy(lin2.at[q, :, aligned(peer2[n], nj), lanes], vin2.at[:, aligned(peer2[n], nj), :], load_sem.at[n + 1])
               for n in range(n2 - 1)])

        @pl.loop(0, ic // 2)
        def _(b):
            rhs_mat = jnp.concatenate([vin2[2 * b], vin2[2 * b + 1]], axis=1)
            res = jnp.dot(mat[...], rhs_mat, preferred_element_type=F32).astype(BF16)
            vout2[2 * b] = res[:, :LANES]
            vout2[2 * b + 1] = res[:, LANES:]

        stores = [pltpu.make_async_copy(vout2.at[:, aligned(peer2[n], nj), :], out2.at[q, :, aligned(peer2[n], nj), lanes], store_sem.at[n + 1])
                  for n in range(n2 - 1)]
        if not last:
            stores += [pltpu.make_async_copy(vout2.at[:, aligned(me2, nj), :], t2.at[q, aligned(me2, ic), :, lanes], store_sem.at[0])]
        run(stores)

    def products(stage, r):
        wait_out_y(stage, r)

        @pl.loop(0, halves)
        def _(h):
            product_one(stage, r, h, False)

        start_back_y(stage, r)
        wait_out_x(stage, r)

        @pl.loop(0, halves)
        def _(h):
            product_two(stage, r, h, False)

        start_back_x(stage, r)

    def third(stage, h, put):
        mat = (ma3, mb3)[stage]
        rows = pl.ds(pl.multiple_of(me3 * nk + h * LANES, LANES), LANES)
        mat_own = mat[rows, aligned(me3, nk)]
        mat_par = mat[rows, aligned(peer3, nk)]
        contract = (((1,), (1,)), ((), ()))
        part = 8

        @pl.loop(0, ni // part)
        def _(b):
            sel = pl.ds(b * part, part)
            term = lax.dot_general(vown[sel].reshape(part * nj, nk), mat_own, contract, preferred_element_type=F32)
            term += lax.dot_general(vpar[sel].reshape(part * nj, nk), mat_par, contract, preferred_element_type=F32)
            put(sel, term.astype(BF16).astype(F32).reshape(part, nj, LANES))

    def load_field(stage, r):
        return [pltpu.make_async_copy(field(stage, r), vown, load_sem.at[2]),
                pltpu.make_async_copy(lin3.at[stage * rhs + r], vpar, load_sem.at[3])]

    def load_terms(stage, r, h):
        q, lanes = stage * rhs + r, aligned(h, LANES)
        return [pltpu.make_async_copy(t1.at[q, :, :, lanes], v1, load_sem.at[0]), pltpu.make_async_copy(t2.at[q, :, :, lanes], v2, load_sem.at[1])]

    def total_a(r, h):
        lanes = aligned(h, LANES)
        run(load_terms(0, r, h) + load_field(0, r) + [pltpu.make_async_copy(d_ref.at[:, :, lanes], vd, load_sem.at[4])])

        def put(sel, term):
            acc = v1[sel].astype(F32) + v2[sel].astype(F32) + term
            vw[sel] = (vd[sel] * acc.astype(BF16).astype(F32)).astype(BF16)

        third(0, h, put)
        run([pltpu.make_async_copy(vw, w.at[r, :, :, lanes], store_sem.at[0])])

    def third_b(r, h):
        run(load_field(1, r))

        def put(sel, term):
            z_ref[r, sel, :, aligned(h, LANES)] = term

        third(1, h, put)

    def total_b(r, h):
        run(load_terms(1, r, h))
        part = 8

        @pl.loop(0, ni // part)
        def _(b):
            sel = pl.ds(b * part, part)
            z_ref[r, sel, :, aligned(h, LANES)] = (v1[sel].astype(F32) + v2[sel].astype(F32)) + z_ref[r, sel, :, aligned(h, LANES)]

    def total_last(r, h):
        lanes = pl.ds(h * LANES, LANES)
        third_b(r, h)
        part = 16

        @pl.loop(0, ni // part)
        def _(b):
            last1[pl.ds(b * part, part), aligned(me1, jc), :] = vout1[pl.ds(me1 * ni + b * part, part)]

        @pl.loop(0, ic // part)
        def _(b):
            last2[pl.ds(me2 * ic + b * part, part)] = vout2[pl.ds(b * part, part), aligned(me2, nj), :]

        def tile(i_block, cols, part):
            @pl.loop(0, ic // part)
            def _(b):
                sel = pl.ds(i_block * ic + b * part, part)
                z_ref[r, sel, cols, lanes] = (last1[sel, cols, :].astype(F32) + last2[sel, cols, :].astype(F32)) + z_ref[r, sel, cols, lanes]

        @pl.loop(0, rhs)
        def _(e):
            wait_out_sends(0, e)
            wait_out_sends(1, e)
            wait_back_sends(0, e)

        @pl.loop(0, rhs - 1)
        def _(e):
            wait_back_sends(1, e)

        @pl.loop(0, halves - 1)
        def _(e):
            wait_back_sends(1, r, e)

        j_blocks = [me1] + [peer1[n1 - 2 - n] for n in order1]
        i_blocks = [me2] + [peer2[n2 - 2 - n] for n in order2]
        for m in range(max(n1, n2)):
            if m < n1:
                if m > 0:
                    back_y(1, r, order1[m - 1], h).wait_recv()
                for e in range(min(m, n2)):
                    tile(i_blocks[e], aligned(j_blocks[m], jc), part)
            if m < n2:
                if m > 0:
                    back_x(1, r, order2[m - 1], h).wait_recv()
                if m + 1 >= n1:
                    tile(i_blocks[m], slice(None), part // 2)
                else:
                    for e in range(m + 1):
                        tile(i_blocks[m], aligned(j_blocks[e], jc), part)
        wait_back_sends(1, r, h)

    @pl.loop(0, rhs)
    def _(r):
        start_out(0, r)

    run([pltpu.make_async_copy(src, dst, mat_sem.at[m]) for m, (src, dst) in enumerate(
        zip((a1_ref, a2_ref, a3_ref, b1_ref, b2_ref, b3_ref), (ma1, ma2, ma3, mb1, mb2, mb3)))])

    @pl.loop(0, rhs)
    def _(r):
        products(0, r)

    @pl.loop(0, rhs)
    def _(r):
        out_c(0, r).wait_recv()
        wait_back(0, r)

        @pl.loop(0, halves)
        def _(h):
            total_a(r, h)

        start_out(1, r)

    @pl.loop(0, rhs - 1)
    def _(r):
        products(1, r)

    end = rhs - 1
    wait_out_y(1, end)
    wait_out_x(1, end)

    @pl.loop(0, halves - 1)
    def _(h):
        product_one(1, end, h, False)
        start_back_y(1, end, h)
        product_two(1, end, h, False)
        start_back_x(1, end, h)

    product_one(1, end, halves - 1, True)
    start_back_y(1, end, halves - 1)
    product_two(1, end, halves - 1, True)
    start_back_x(1, end, halves - 1)

    @pl.loop(0, rhs)
    def _(r):
        out_c(1, r).wait_recv()

    @pl.loop(0, rhs - 1)
    def _(r):
        @pl.loop(0, halves)
        def _(h):
            third_b(r, h)

        wait_back(1, r)

        @pl.loop(0, halves)
        def _(h):
            total_b(r, h)

    @pl.loop(0, halves - 1)
    def _(h):
        third_b(end, h)
        wait_back(1, end, h)
        total_b(end, h)

    total_last(end, halves - 1)


def write_out(z_in, z_out, sem):
    rhs, parts = sem.shape
    size = z_in.shape[1] // parts
    copies = [pltpu.make_async_copy(z_in.at[r, pl.ds(b * size, size)], z_out.at[r, pl.ds(b * size, size)], sem.at[r, b])
              for r in range(rhs) for b in range(parts)]
    for copy in copies:
        copy.start()
    for copy in copies:
        copy.wait()


def solution(mesh):
    n1, n2, n3 = mesh.shape['mode1'], mesh.shape['mode2'], mesh.shape['mode3']
    vol_spec = P('rhs', 'mode1', 'mode2', 'mode3')
    diag_spec = P('mode1', 'mode2', 'mode3')

    def local_op(x_vol, diag_vals, *mats):
        rhs, ni, nj, nk = x_vol.shape
        dims = (n1, n2, n3, rhs, ni, nj, nk)
        halves = nk // LANES
        backs = 2 * rhs - 1 + halves
        jc, ic = nj // n1, ni // n2
        hbm = pl.BlockSpec(memory_space=pltpu.HBM)
        vmem = pl.BlockSpec(memory_space=pltpu.VMEM)
        dma = pltpu.SemaphoreType.DMA
        block = (ni, nj, LANES)
        outs = [
            pltpu.VMEM(x_vol.shape, F32),
            jax.ShapeDtypeStruct((2 * rhs, n1 * ni, jc, nk), BF16),
            jax.ShapeDtypeStruct((2 * rhs, ic, n2 * nj, nk), BF16),
            jax.ShapeDtypeStruct((2 * rhs, ni, nj, nk), BF16),
            jax.ShapeDtypeStruct((2 * rhs, n1 * ni, jc, nk), BF16),
            jax.ShapeDtypeStruct((2 * rhs, ic, n2 * nj, nk), BF16),
            jax.ShapeDtypeStruct((2 * rhs, ni, nj, nk), BF16),
            jax.ShapeDtypeStruct((2 * rhs, ni, nj, nk), BF16),
            jax.ShapeDtypeStruct(x_vol.shape, BF16),
        ]
        scratch = [pltpu.VMEM(mat.shape, mat.dtype) for mat in mats] + [
            pltpu.VMEM((n1 * ni, jc, LANES), BF16),
            pltpu.VMEM((n1 * ni * jc, LANES), F32),
            pltpu.VMEM((n1 * ni, jc, LANES), BF16),
            pltpu.VMEM((ic, n2 * nj, LANES), BF16),
            pltpu.VMEM((ic, n2 * nj, LANES), BF16),
            pltpu.VMEM(block, BF16),
            pltpu.VMEM(block, BF16),
            pltpu.VMEM((ni, nj, nk), BF16),
            pltpu.VMEM((ni, nj, nk), BF16),
            pltpu.VMEM(block, F32),
            pltpu.VMEM(block, BF16),
            pltpu.VMEM(block, BF16),
            pltpu.VMEM(block, BF16),
            dma((2 * rhs, n1 - 1)), dma((2 * rhs, n1 - 1)),
            dma((2 * rhs, n2 - 1)), dma((2 * rhs, n2 - 1)),
            dma((2 * rhs,)), dma((2 * rhs,)),
            dma((backs, n1 - 1)), dma((backs, n1 - 1)),
            dma((backs, n2 - 1)), dma((backs, n2 - 1)),
            dma((len(mats),)), dma((max(5, n1, n2),)), dma((max(n1, n2),)),
        ]
        z_vol = pl.pallas_call(
            functools.partial(kernel, dims),
            out_shape=outs,
            in_specs=[hbm] * (2 + len(mats)),
            out_specs=[vmem] + [hbm] * (len(outs) - 1),
            scratch_shapes=scratch,
            compiler_params=pltpu.CompilerParams(collective_id=0, has_side_effects=True, vmem_limit_bytes=46 * 2 ** 20),
        )(x_vol, diag_vals, *mats)[0]
        return pl.pallas_call(
            write_out,
            out_shape=jax.ShapeDtypeStruct(x_vol.shape, F32),
            in_specs=[vmem],
            out_specs=hbm,
            scratch_shapes=[dma((rhs, 4))],
            compiler_params=pltpu.CompilerParams(vmem_limit_bytes=24 * 2 ** 20),
        )(z_vol)

    return jax.shard_map(local_op, mesh=mesh, in_specs=(vol_spec, diag_spec, P(), P(), P(), P(), P(), P()), out_specs=vol_spec, check_vma=False)
```
